256 devices in a mesh: groups: 2 (over z), dev: 16 (over y, core), tp: 8 (over x).
Axes of the slice: x: 8, y: 8, z: 2, core: 2. Of those that a mesh axis runs over, the one named last changes fastest.
The devices are a block of a 8x8x16 slice.
Arguments:
- hidden_states: bfloat16 [20480, 5120], P(('groups', 'dev'), 'tp'), parts along dimension 0, may hold values from -6 to 6
- norm_gain: bfloat16 [5120], replicated, may hold values from 0.25 to 1.75
- w_query: bfloat16 [5120, 5120], P('dev', 'tp'), may hold values from -2 to 2
- w_key: bfloat16 [5120, 1024], P('dev', 'tp'), may hold values from -2 to 2
- w_value: bfloat16 [5120, 1024], P('dev', 'tp'), may hold values from -0.078125 to 0.078125
- prompt_blocks: int32 [16], P('groups'), parts along dimension 0, may hold values from 1 to 11, 80 in all
- owner_map: int32 [160], P(('groups', 'dev')), parts along dimension 0, may hold values from 0 to 15, as said below
- slot_table: int32 [32, 32], P(('groups', 'dev')), parts along dimension 0, may hold values from 0 to 31, each once within a row
Outputs:
- context: bfloat16 [20480, 5120], P(('groups', 'dev'), 'tp'), parts along dimension 0
- kv_cache: bfloat16 [1024, 128, 2048], P(('groups', 'dev'), None, 'tp'), parts along dimension 0
The draws below stay inside these ranges and needn't reach their ends.
There are 2 independent parts, one for each index of `groups`. The reference program is written for one: setup_inputs(seed, part) draws one part's arguments, and reference() takes and returns one part's arrays. A program takes and returns all parts, laid end to end along the dimension named above; an argument that names none is the same for every part. Nothing has to cross between parts.
Inputs may be any that keep to these rules, and one draw needn't show every extreme that they name: `prompt_blocks`: the entries sum to 80. `owner_map`: each device's 5 blocks name any owner at most 2 times, and no owner receives more than 32 blocks; in every draw some owner receives 2 blocks from every device. `slot_table`: each row is a permutation of 0 to 31.
All inputs are finite; a program needn't handle non-finite values.
Results may differ from the reference program's by a relative error of at most 0.0079.
Values may be sent and summed in bfloat16 or wider, within the bound.
No kernel may reach another device: no remote copies, remote signals or barrier semaphores. Data moves between devices by JAX's collectives and lax.ppermute only.
A program may use at most 128 MiB of HBM per device.

```python
import math
import jax
import jax.numpy as jnp
import numpy as np
from jax import lax

D = 5120
HD = 128
KV_HEADS = 8
HEADS = 40
BLOCK = 128
PROMPTS = 8
PAIR_CAP = 2
TOKENS = 10240
BLK_DEV = 5
BLOCKS = 80
LEN_BLOCKS = 11
SLOTS = 32
N_DEV = 16


def joint_weights(key):
    base = jax.random.fold_in(key, 7171)
    factor = D ** (-0.5)
    group_size = HEADS // KV_HEADS
    key_part = jax.random.truncated_normal(jax.random.fold_in(base, 1), -4.0, 4.0, (D, KV_HEADS, HD), jnp.float32) * factor
    query_part = jax.random.truncated_normal(jax.random.fold_in(base, 4), -4.0, 4.0, (D, KV_HEADS, group_size, HD), jnp.float32) * factor
    return (query_part.reshape(D, HEADS * HD), key_part.reshape(D, KV_HEADS * HD))


def draw_w_query(key, part):
    return joint_weights(key)[0].astype(jnp.bfloat16)


def draw_w_key(key, part):
    return joint_weights(key)[1].astype(jnp.bfloat16)


def draw_owner_map(key, part):
    hottest = jax.random.randint(jax.random.fold_in(key, 5), (), 0, N_DEV)

    def one_device(device):
        stream = jax.random.fold_in(key, 100 + device)
        first_pass = jax.random.permutation(jax.random.fold_in(stream, 1), N_DEV - 1)
        second_pass = jax.random.permutation(jax.random.fold_in(stream, 2), N_DEV - 1)
        others = jnp.concatenate([first_pass, second_pass])[:BLK_DEV - PAIR_CAP]
        others = others + (others >= hottest).astype(jnp.int32)
        picks = jnp.concatenate([jnp.full((PAIR_CAP,), hottest, jnp.int32), others.astype(jnp.int32)])
        shuffle = jax.random.permutation(jax.random.fold_in(stream, 3), BLK_DEV)
        return picks[shuffle]
    return jax.vmap(one_device)(jnp.arange(N_DEV, dtype=jnp.int32)).reshape(-1).astype(jnp.int32)


def shard_levels(stream_key, dims, cuts, low, largest):
    loudness, own = 1.0, jax.random.fold_in(stream_key, 6)
    for axis_at, shards_of in cuts:
        draws = jnp.exp(jax.random.uniform(jax.random.fold_in(own, axis_at), (shards_of,), jnp.float32, low / len(cuts), largest / len(cuts)))
        loudness = loudness * jnp.repeat(draws, dims[axis_at] // shards_of).reshape([-1 if axis == axis_at else 1 for axis in range(len(dims))])
    return loudness


def length_profile(count, total, limit, lean):
    weights = [(1 << 20) // math.isqrt(standing ** lean) + 1 for standing in range(2, count + 1)]
    surplus, counts = total - limit - (count - 1), [1] * (count - 1)
    while surplus > 0:
        free = [i for i in range(count - 1) if counts[i] < limit]
        mass, budget = sum([weights[i] for i in free]), surplus
        for i in free:
            extra = min(limit - counts[i], max(1, budget * weights[i] // mass), surplus)
            counts[i] = counts[i] + extra
            surplus = surplus - extra
    return np.array([limit] + counts)


def uneven(stream_key, amount, total, most, lean):
    if amount == 2:
        one = jax.random.randint(stream_key, (), max(1, total - most), min(most, total - 1) + 1)
        return jnp.stack([one, total - one])
    sizes = jnp.asarray(length_profile(amount, total, most, lean), jnp.int32)
    twos = (amount - 1) // 2
    donor, taker = sizes[1:1 + 2 * twos:2], sizes[2:2 + 2 * twos:2]
    room = jnp.minimum(donor - 1, most - taker)
    moved = jax.random.randint(jax.random.fold_in(stream_key, 1), (twos,), 0, 1 << 20) % (room + 1)
    sizes = sizes.at[1:1 + 2 * twos:2].set(donor - moved).at[2:2 + 2 * twos:2].set(taker + moved)
    return sizes[jax.random.permutation(jax.random.fold_in(stream_key, 2), amount)]


def bell_draw(key, shape, deviation, limit, cuts=(), kind=jnp.bfloat16):
    values = deviation * jax.random.normal(key, shape, jnp.float32)
    if cuts:
        values = values * shard_levels(key, shape, cuts, -0.22, 0.18)
    return jnp.clip(values, -limit, limit).astype(kind)


def setup_inputs(seed: int = 0, part: int = 0) -> dict:
    seeds = jax.random.split(jax.random.key(seed), 9)
    part_splits = jax.random.split(jax.random.fold_in(seeds[8], part), 9)
    hidden_states = bell_draw(part_splits[0], (TOKENS, D), 1.0, 6.0, ((0, 16), (1, 8)))
    norm_gain = jnp.clip(1.0 + 0.15 * jax.random.normal(seeds[1], (D,), jnp.float32), 0.25, 1.75).astype(jnp.bfloat16)
    w_query = draw_w_query(jax.random.fold_in(seeds[8], 71), part)
    w_key = draw_w_key(jax.random.fold_in(seeds[8], 71), part)
    w_value = bell_draw(seeds[4], (D, KV_HEADS * HD), D ** -0.5, 0.078125, ((0, 16), (1, 8)))
    prompt_blocks = uneven(part_splits[5], PROMPTS, BLOCKS, LEN_BLOCKS, 2).astype(jnp.int32)
    owner_map = draw_owner_map(jax.random.fold_in(jax.random.fold_in(seeds[8], part), 71), part)
    slot_table = jax.vmap(lambda own: jax.random.permutation(own, SLOTS))(jax.random.split(part_splits[7], N_DEV)).reshape((N_DEV, SLOTS)).astype(jnp.int32)
    return {"hidden_states": hidden_states, "norm_gain": norm_gain, "w_query": w_query, "w_key": w_key, "w_value": w_value, "prompt_blocks": prompt_blocks, "owner_map": owner_map, "slot_table": slot_table}


EPSILON = 1e-06
THETA = 1000000.0

def prompt_start(positions, starts):
    return lax.optimization_barrier(jnp.max(jnp.where(positions[:, None] >= starts[None, :], starts[None, :], 0), axis=1))

def rotate(heads, offsets):
    half_width = heads.shape[-1] // 2
    freq_index = jnp.arange(half_width, dtype=jnp.float32)
    inverse = jnp.exp(freq_index * (-2.0 * math.log(THETA) / heads.shape[-1]))
    angles = offsets.astype(jnp.float32)[:, None] * inverse[None, :]
    cosine = jnp.cos(angles)[:, None, :]
    sine_part = jnp.sin(angles)[:, None, :]
    first_half = heads[..., :half_width]
    second = heads[..., half_width:]
    return jnp.concatenate([first_half * cosine - second * sine_part, second * cosine + first_half * sine_part], axis=-1)

def reference(hidden_states, norm_gain, w_query, w_key, w_value, prompt_blocks, owner_map, slot_table):
    floats = hidden_states.astype(jnp.float32)
    square = lax.optimization_barrier(jnp.mean(floats * floats, axis=1, keepdims=True))
    normed = (floats * lax.rsqrt(square + EPSILON) * norm_gain.astype(jnp.float32)).astype(jnp.bfloat16)
    query_proj = jnp.dot(normed, w_query, preferred_element_type=jnp.float32)
    key_proj = jnp.dot(normed, w_key, preferred_element_type=jnp.float32)
    value_proj = jnp.dot(normed, w_value, preferred_element_type=jnp.float32)
    group_size = HEADS // KV_HEADS
    token_rows = jnp.arange(TOKENS, dtype=jnp.int32)
    starts = ((jnp.cumsum(prompt_blocks) - prompt_blocks) * BLOCK).astype(jnp.int32)
    start_of = prompt_start(token_rows, starts)
    offsets = token_rows - start_of
    queries = rotate(query_proj.reshape(TOKENS, HEADS, HD), offsets).astype(jnp.bfloat16)
    rope_keys = rotate(key_proj.reshape(TOKENS, KV_HEADS, HD), offsets).astype(jnp.bfloat16)
    values = value_proj.reshape(TOKENS, KV_HEADS, HD).astype(jnp.bfloat16)
    window = LEN_BLOCKS * BLOCK + BLOCK
    score_scale = 1.0 / math.sqrt(HD)

    def one_block(block_index):
        first_row = (block_index * BLOCK).astype(jnp.int32)
        window_start = jnp.maximum(first_row + BLOCK - window, 0).astype(jnp.int32)
        block_queries = lax.dynamic_slice_in_dim(queries, first_row, BLOCK, 0).astype(jnp.float32)
        block_queries = block_queries.reshape(BLOCK, KV_HEADS, group_size, HD)
        block_keys = lax.dynamic_slice_in_dim(rope_keys, window_start, window, 0).astype(jnp.float32)
        block_values = lax.dynamic_slice_in_dim(values, window_start, window, 0).astype(jnp.float32)
        query_rows = first_row + jnp.arange(BLOCK, dtype=jnp.int32)
        key_rows = window_start + jnp.arange(window, dtype=jnp.int32)
        query_start = lax.dynamic_slice_in_dim(start_of, first_row, BLOCK, 0)
        key_start = lax.dynamic_slice_in_dim(start_of, window_start, window, 0)
        allowed = (query_start[:, None] == key_start[None, :]) & (key_rows[None, :] <= query_rows[:, None])
        allowed_heads = allowed[:, None, None, :]
        scores = jnp.einsum('tkgd,wkd->tkgw', block_queries, block_keys) * score_scale
        scores = jnp.where(allowed_heads, scores, -1e+30)
        row_max = lax.optimization_barrier(jnp.max(scores, axis=-1, keepdims=True))
        weights = jnp.where(allowed_heads, jnp.exp(scores - row_max), 0.0)
        row_total = lax.optimization_barrier(jnp.sum(weights, axis=-1))
        rounded = lax.optimization_barrier(weights.astype(jnp.bfloat16)).astype(jnp.float32)
        weighted = jnp.einsum('tkgw,wkd->tkgd', rounded, block_values)
        return (weighted / row_total[..., None]).reshape(BLOCK, HEADS * HD).astype(jnp.bfloat16)
    context = lax.map(one_block, jnp.arange(TOKENS // BLOCK, dtype=jnp.int32)).reshape(TOKENS, HEADS * HD)
    owner_hits = (owner_map[:, None] == jnp.arange(N_DEV, dtype=jnp.int32)[None, :]).astype(jnp.int32)
    earlier_hits = jnp.cumsum(owner_hits, axis=0) - owner_hits
    ranks = lax.optimization_barrier(jnp.sum(earlier_hits * owner_hits, axis=1)).astype(jnp.int32)
    slots = slot_table[owner_map, ranks]
    target = (owner_map * SLOTS + slots).astype(jnp.int32)
    packed = jnp.stack([rope_keys, values], axis=2).reshape(BLOCKS, BLOCK, 2 * KV_HEADS * HD)
    kv_cache = jnp.zeros((N_DEV * SLOTS, BLOCK, 2 * KV_HEADS * HD), jnp.bfloat16).at[target].set(packed)
    return (context, kv_cache)
```

```python
import functools
import math

import jax
import jax.numpy as jnp
from jax import lax
from jax.experimental import pallas as pl
from jax.experimental.pallas import tpu as pltpu
from jax.sharding import PartitionSpec as P

HD = 128
BLOCK = 128
LEN_BLOCKS = 11
EPSILON = 1e-06
THETA = 1000000.0
HBM = pltpu.MemorySpace.HBM
VMEM = pltpu.MemorySpace.VMEM
SMEM = pltpu.MemorySpace.SMEM


def ring(block, axis, hop):
    size = lax.axis_size(axis)
    count = size // hop
    ahead = [(i, (i + hop) % size) for i in range(size)]
    back = [(i, (i - hop) % size) for i in range(size)]
    got = {0: block}
    up = down = block
    for step in range(1, count // 2):
        up = lax.ppermute(up, axis, ahead)
        down = lax.ppermute(down, axis, back)
        got[count - step] = up
        got[step] = down
    half = block.shape[0] // 2
    top = lax.ppermute(up[:half], axis, ahead)
    bottom = lax.ppermute(down[half:], axis, back)
    return got, (top, bottom)


def swap(block, axis):
    size = lax.axis_size(axis)
    return lax.ppermute(block, axis, [(i, i ^ 1) for i in range(size)])


def proj_kernel(
    place, *refs, count, rows, feat, width, lo, n_q, n_kv, has_old
):
    count_x = count + 1
    x_refs = refs[:count_x]
    mine, other, gain, cos, sin = refs[count_x : count_x + 5]
    at = count_x + 5
    old = None
    if has_old:
        old = refs[at]
        at += 1
    n_out = (1 if n_q else 0) + (1 if n_kv else 0)
    outs = refs[at : at + n_out]
    xbuf, wbuf, acc, sq, sem_x, sem_w = refs[at + n_out :]
    tp, chip, core = place[0], place[1], place[2]
    w_rows = feat // 2
    half = rows // 2
    mid = count // 2

    def x_copies():
        copies = []
        for i in range(count):
            if i == mid:
                copies.append(pltpu.make_async_copy(x_refs[i], xbuf.at[i, pl.ds(0, half)], sem_x.at[i]))
                copies.append(
                    pltpu.make_async_copy(x_refs[count], xbuf.at[i, pl.ds(half, half)], sem_x.at[count])
                )
            else:
                copies.append(pltpu.make_async_copy(x_refs[i], xbuf.at[i], sem_x.at[i]))
        return copies

    def w_copy(i, which):
        src = mine if which == 0 else other
        spot = core if which == 0 else 1 - core
        rel = lax.rem(tp + i - chip + count, count)
        return pltpu.make_async_copy(
            src.at[rel, :, pl.ds(lo, width)],
            wbuf.at[i, pl.ds(pl.multiple_of(spot * w_rows, 64), w_rows)],
            sem_w.at[2 * i + which],
        )

    copies = x_copies()
    for i in range(count):
        copies[i if i <= mid else i + 1].start()
        if i == mid:
            copies[mid + 1].start()
        w_copy(i, 0).start()
        w_copy(i, 1).start()
    acc[...] = jnp.zeros_like(acc)
    sq[...] = jnp.zeros_like(sq)
    for i in range(count):
        copies[i if i <= mid else i + 1].wait()
        if i == mid:
            copies[mid + 1].wait()
        w_copy(i, 0).wait()
        w_copy(i, 1).wait()
        feature = lax.rem(tp + i, count)
        x = xbuf[i].astype(jnp.float32)
        xx = x * x
        total = xx[:, :128]
        for g in range(1, feat // 128):
            total = total + xx[:, g * 128 : (g + 1) * 128]
        sq[...] += total
        scaled = (x * gain[pl.ds(feature, 1), :]).astype(jnp.bfloat16)
        acc[...] += jnp.dot(scaled, wbuf[i], preferred_element_type=jnp.float32)
    mean = jnp.sum(sq[...], axis=1, keepdims=True) * (1.0 / (feat * count))
    scale = lax.rsqrt(mean + EPSILON)
    cosine = cos[...]
    sine = sin[...]

    def rotated(at_col):
        head = acc[:, at_col : at_col + HD] * scale
        return (head * cosine + pltpu.roll(head, HD // 2, 1) * sine).astype(jnp.bfloat16)

    for h in range(n_q):
        outs[0][h] = rotated(h * HD)
    if n_kv:
        kv = outs[-1]
        base = 0
        if has_old:
            base = old.shape[0]
            kv[:base] = old[...]
        k_at = n_q * HD
        kv[base : base + rows, :HD] = rotated(k_at)
        kv[base : base + rows, HD:] = (acc[:, k_at + HD : k_at + 2 * HD] * scale).astype(jnp.bfloat16)


def project(place, got, halves, mine, other, gain, cos, sin, n_q, kv, lo, old=None):
    count = len(got) + 1
    rows, feat = got[0].shape
    mid = count // 2
    pieces = [got[i] if i != mid else halves[0] for i in range(count)] + [halves[1]]
    width = n_q * HD + (2 * HD if kv else 0)
    outs = []
    if n_q:
        outs.append(jax.ShapeDtypeStruct((n_q, rows, HD), jnp.bfloat16))
    if kv:
        outs.append(
            jax.ShapeDtypeStruct((rows + (old.shape[0] if old is not None else 0), 2 * HD), jnp.bfloat16)
        )
    kernel = functools.partial(
        proj_kernel,
        count=count,
        rows=rows,
        feat=feat,
        width=width,
        lo=lo,
        n_q=n_q,
        n_kv=1 if kv else 0,
        has_old=old is not None,
    )
    operands = [place, *pieces, mine, other, gain, cos, sin]
    specs = [pl.BlockSpec(memory_space=SMEM)]
    specs += [pl.BlockSpec(memory_space=HBM)] * (len(pieces) + 2)
    specs += [pl.BlockSpec(memory_space=VMEM)] * 3
    if old is not None:
        operands.append(old)
        specs.append(pl.BlockSpec(memory_space=VMEM))
    flops = 2 * rows * feat * count * width
    return pl.pallas_call(
        kernel,
        out_shape=tuple(outs),
        in_specs=specs,
        out_specs=tuple(pl.BlockSpec(memory_space=VMEM) for _ in outs),
        scratch_shapes=[
            pltpu.VMEM((count, rows, feat), jnp.bfloat16),
            pltpu.VMEM((count, feat, width), jnp.bfloat16),
            pltpu.VMEM((rows, width), jnp.float32),
            pltpu.VMEM((rows, 128), jnp.float32),
            pltpu.SemaphoreType.DMA((count + 1,)),
            pltpu.SemaphoreType.DMA((2 * count,)),
        ],
        compiler_params=pltpu.CompilerParams(vmem_limit_bytes=48 * 1024 * 1024),
        cost_estimate=pl.CostEstimate(
            flops=flops, bytes_accessed=2 * feat * count * (width + rows), transcendentals=0
        ),
    )(*operands)


def attend_kernel(info, q_a, q_b, far, near, own, out, qbuf, kvbuf, sbuf, mbuf, lbuf, obuf, sems):
    heads, part, _ = q_a.shape
    tok = own.shape[0]
    local = tok // BLOCK
    back = 2 * local
    copies = [
        pltpu.make_async_copy(q_a, qbuf.at[:, pl.ds(0, part)], sems.at[0]),
        pltpu.make_async_copy(q_b, qbuf.at[:, pl.ds(part, tok - part)], sems.at[1]),
        pltpu.make_async_copy(far, kvbuf.at[pl.ds(0, tok)], sems.at[2]),
        pltpu.make_async_copy(near, kvbuf.at[pl.ds(tok, tok)], sems.at[3]),
        pltpu.make_async_copy(own, kvbuf.at[pl.ds(2 * tok, tok)], sems.at[4]),
    ]
    for copy in copies:
        copy.start()
    for copy in copies:
        copy.wait()
    first = info[0]
    n_prompts = info.shape[0] - 1
    factor = math.log2(math.e) / math.sqrt(HD)
    row = lax.broadcasted_iota(jnp.int32, (heads * BLOCK, BLOCK), 0)
    col = lax.broadcasted_iota(jnp.int32, (heads * BLOCK, BLOCK), 1)
    causal = col <= jnp.bitwise_and(row, BLOCK - 1)

    def one_block(i, unused):
        block = first + i

        def find(p, state):
            start, best = state
            best = jnp.where(start <= block, start, best)
            return start + info[1 + p], best

        _, begin = lax.fori_loop(0, n_prompts, find, (jnp.int32(0), jnp.int32(0)))
        low = jnp.maximum(begin - first + back, i)
        q = qbuf[:, pl.ds(pl.multiple_of(i * BLOCK, BLOCK), BLOCK), :].reshape(heads * BLOCK, HD)

        def score(j):
            keys = kvbuf[pl.ds(pl.multiple_of(j * BLOCK, BLOCK), BLOCK), :HD]
            return lax.dot_general(
                q, keys, (((1,), (1,)), ((), ())), preferred_element_type=jnp.float32
            )

        last = back + i
        s = jnp.where(causal, score(last), -1e30)
        sbuf[last] = s
        mbuf[...] = s

        def upward(j, unused):
            s = score(j)
            sbuf[j] = s
            mbuf[...] = jnp.maximum(mbuf[...], s)
            return unused

        lax.fori_loop(low, last, upward, 0)
        top = jnp.max(mbuf[...], axis=1, keepdims=True)
        mbuf[...] = jnp.broadcast_to(top, mbuf.shape)
        lbuf[...] = jnp.zeros_like(lbuf)
        obuf[...] = jnp.zeros_like(obuf)

        def gather(j, unused):
            p = jnp.exp2((sbuf[j] - mbuf[...]) * factor)
            lbuf[...] += p
            vals = kvbuf[pl.ds(pl.multiple_of(j * BLOCK, BLOCK), BLOCK), HD:]
            obuf[...] += jnp.dot(p.astype(jnp.bfloat16), vals, preferred_element_type=jnp.float32)
            return unused

        lax.fori_loop(low, last + 1, gather, 0)
        total = jnp.sum(lbuf[...], axis=1, keepdims=True)
        result = (obuf[...] / total).astype(jnp.bfloat16)
        at = pl.ds(pl.multiple_of(i * BLOCK, BLOCK), BLOCK)
        for h in range(heads):
            out[at, h * HD : (h + 1) * HD] = result[h * BLOCK : (h + 1) * BLOCK]
        return unused

    lax.fori_loop(0, local, one_block, 0)


def attend(info, q_a, q_b, far, near, own):
    heads = q_a.shape[0]
    tok = own.shape[0]
    tiles = 3 * tok // BLOCK
    return pl.pallas_call(
        attend_kernel,
        out_shape=jax.ShapeDtypeStruct((tok, heads * HD), jnp.bfloat16),
        in_specs=[pl.BlockSpec(memory_space=SMEM)] + [pl.BlockSpec(memory_space=HBM)] * 5,
        out_specs=pl.BlockSpec(memory_space=VMEM),
        scratch_shapes=[
            pltpu.VMEM((heads, tok, HD), jnp.bfloat16),
            pltpu.VMEM((3 * tok, 2 * HD), jnp.bfloat16),
            pltpu.VMEM((tiles, heads * BLOCK, BLOCK), jnp.float32),
            pltpu.VMEM((heads * BLOCK, BLOCK), jnp.float32),
            pltpu.VMEM((heads * BLOCK, BLOCK), jnp.float32),
            pltpu.VMEM((heads * BLOCK, HD), jnp.float32),
            pltpu.SemaphoreType.DMA((5,)),
        ],
        compiler_params=pltpu.CompilerParams(vmem_limit_bytes=32 * 1024 * 1024),
        cost_estimate=pl.CostEstimate(
            flops=12 * 10**9, bytes_accessed=4 * 10**6, transcendentals=10**6
        ),
    )(info, q_a, q_b, far, near, own)


def cache_kernel(place, owners, table, mine, other, mine_mid, other_mid, out, sem, *, local, count, tok):
    chip, core, me = place[1], place[2], place[3]
    mid = count // 2
    blocks = owners.shape[0]
    slots = out.shape[0]

    def put(src, at_row, slot):
        return pltpu.make_async_copy(src.at[pl.ds(pl.multiple_of(at_row, BLOCK), BLOCK)], out.at[slot], sem)

    def one(b, rank):
        hit = owners[b] == me

        @pl.when(hit)
        def _():
            slot = table[0, rank]
            source = b // local
            rel = lax.rem(source // 2 - chip + count, count)
            same = lax.rem(source, 2) == core
            inner = lax.rem(b, local) * BLOCK
            middle = rel == mid
            spot = jnp.where(rel > mid, rel - 1, jnp.where(middle, 0, rel))
            at_row = spot * tok + inner

            @pl.when(same & jnp.logical_not(middle))
            def _():
                put(mine, at_row, slot).start()

            @pl.when(jnp.logical_not(same) & jnp.logical_not(middle))
            def _():
                put(other, at_row, slot).start()

            @pl.when(same & middle)
            def _():
                put(mine_mid, at_row, slot).start()

            @pl.when(jnp.logical_not(same) & middle)
            def _():
                put(other_mid, at_row, slot).start()

        return rank + hit.astype(jnp.int32)

    found = lax.fori_loop(0, blocks, one, jnp.int32(0))

    def clear(r, unused):
        out[table[0, r]] = jnp.zeros(out.shape[1:], out.dtype)
        return unused

    lax.fori_loop(found, slots, clear, 0)

    def settle(r, unused):
        put(mine, 0, 0).wait()
        return unused

    lax.fori_loop(0, found, settle, 0)


def fill_cache(place, owners, table, mine, other, mine_mid, other_mid, local, count):
    tok = mine_mid.shape[0]
    slots = table.shape[1]
    return pl.pallas_call(
        functools.partial(cache_kernel, local=local, count=count, tok=tok),
        out_shape=jax.ShapeDtypeStruct((slots, BLOCK, mine.shape[1]), jnp.bfloat16),
        in_specs=[pl.BlockSpec(memory_space=SMEM)] * 3 + [pl.BlockSpec(memory_space=HBM)] * 4,
        out_specs=pl.BlockSpec(memory_space=VMEM),
        scratch_shapes=[pltpu.SemaphoreType.DMA],
        compiler_params=pltpu.CompilerParams(vmem_limit_bytes=16 * 1024 * 1024),
    )(place, owners, table, mine, other, mine_mid, other_mid)


def on_device(
    hidden_states, norm_gain, w_query, w_key, w_value, prompt_blocks, owner_map, slot_table
):
    tok, feat = hidden_states.shape
    n_dev = lax.axis_size("dev")
    n_tp = lax.axis_size("tp")
    device = lax.axis_index("dev")
    count = n_dev // 2
    local = tok // BLOCK
    heads = w_query.shape[1] // HD
    place = jnp.stack([lax.axis_index("tp"), device // 2, device % 2, device]).astype(jnp.int32)

    part = tok // 2
    x_a, half_a = ring(hidden_states[:part], "tp", 1)
    x_b, half_b = ring(hidden_states[part:], "tp", 1)

    weights = jnp.concatenate([w_query, w_key, w_value], axis=1)
    w_got, w_half = ring(weights, "dev", 2)
    mid = count // 2
    mine = jnp.stack(
        [w_got[i] if i != mid else jnp.concatenate(w_half, axis=0) for i in range(count)]
    )
    other = swap(mine, "dev")
    owners = lax.all_gather(owner_map, "dev", axis=0, tiled=True)

    token_rows = device * tok + jnp.arange(tok, dtype=jnp.int32)
    starts = (jnp.cumsum(prompt_blocks) - prompt_blocks) * BLOCK
    start_of = jnp.max(jnp.where(token_rows[:, None] >= starts[None, :], starts[None, :], 0), axis=1)
    offsets = token_rows - start_of
    freq_index = jnp.arange(HD // 2, dtype=jnp.float32)
    inverse = jnp.exp(freq_index * (-2.0 * math.log(THETA) / HD))
    angles = offsets.astype(jnp.float32)[:, None] * inverse[None, :]
    cosine, sine = jnp.cos(angles), jnp.sin(angles)
    cos = jnp.concatenate([cosine, cosine], axis=1)
    sin = jnp.concatenate([-sine, sine], axis=1)
    gain = norm_gain.astype(jnp.float32).reshape(n_tp, feat)

    q_width = heads * HD
    q_a, kv_a = project(
        place, x_a, half_a, mine, other, gain, cos[:part], sin[:part], heads, True, 0
    )
    (kv,) = project(
        place, x_b, half_b, mine, other, gain, cos[part:], sin[part:], 0, True, q_width, old=kv_a
    )
    (q_b,) = project(
        place, x_b, half_b, mine, other, gain, cos[part:], sin[part:], heads, False, 0
    )

    k_got, k_half = ring(kv, "dev", 2)
    near = lax.ppermute(kv, "dev", [(i, i + 1) for i in range(n_dev - 1)])
    far = k_got[count - 1]
    info = jnp.concatenate([(device * local)[None].astype(jnp.int32), prompt_blocks])
    context = attend(info, q_a, q_b, far, near, kv)
    k_mine = jnp.concatenate([k_got[i] for i in range(count) if i != mid], axis=0)
    k_other = swap(k_mine, "dev")
    k_mid = jnp.concatenate(k_half, axis=0)
    k_mid_other = swap(k_mid, "dev")
    kv_cache = fill_cache(
        place, owners, slot_table, k_mine, k_other, k_mid, k_mid_other, local, count
    )
    return (context, kv_cache)


def solution(mesh):
    in_specs = (
        P(("groups", "dev"), "tp"),
        P(),
        P("dev", "tp"),
        P("dev", "tp"),
        P("dev", "tp"),
        P("groups"),
        P(("groups", "dev")),
        P(("groups", "dev"), None),
    )
    out_specs = (P(("groups", "dev"), "tp"), P(("groups", "dev"), None, "tp"))
    return jax.shard_map(
        on_device, mesh=mesh, in_specs=in_specs, out_specs=out_specs, check_vma=False
    )
```

```python
import functools
import math

import jax
import jax.numpy as jnp
from jax import lax
from jax.experimental import pallas as pl
from jax.experimental.pallas import tpu as pltpu
from jax.sharding import PartitionSpec as P


HD = 128
BLOCK = 128
LEN_BLOCKS = 11
EPSILON = 1e-06
THETA = 1000000.0
VMEM = pltpu.MemorySpace.VMEM
SMEM = pltpu.MemorySpace.SMEM


def ring(block, axis, hop, last_ahead):
    size = lax.axis_size(axis)
    count = size // hop
    ahead = [(i, (i + hop) % size) for i in range(size)]
    back = [(i, (i - hop) % size) for i in range(size)]
    got = {0: block}
    up = down = block
    for step in range(1, count // 2):
        up = lax.ppermute(up, axis, ahead)
        down = lax.ppermute(down, axis, back)
        got[count - step] = up
        got[step] = down
    if last_ahead:
        got[count // 2] = lax.ppermute(up, axis, ahead)
    else:
        got[count // 2] = lax.ppermute(down, axis, back)
    return [got[i] for i in range(count)]


def swap(block, axis):
    size = lax.axis_size(axis)
    return lax.ppermute(block, axis, [(i, i ^ 1) for i in range(size)])


def proj_kernel(place, *refs, count, rows, feat, width, lo, n_q, kv, has_scale, has_old):
    x_refs = refs[:count]
    mine, other, gain, cos, sin = refs[count : count + 5]
    at = count + 5
    old = scale_in = None
    if has_old:
        old = refs[at]
        at += 1
    if has_scale:
        scale_in = refs[at]
        at += 1
    n_out = (1 if n_q else 0) + (1 if kv else 0) + (0 if has_scale else 1)
    outs = refs[at : at + n_out]
    xbuf, wbuf, acc, scale_ref, sem_x, sem_w = refs[at + n_out :]
    tp, chip, core = place[0], place[1], place[2]
    w_rows = feat // 2
    tile = 64

    def x_copy(i):
        return pltpu.make_async_copy(x_refs[i], xbuf.at[:, pl.ds(i * feat, feat)], sem_x.at[i])

    def w_copy(i, which):
        src = mine if which == 0 else other
        spot = core if which == 0 else 1 - core
        rel = lax.rem(tp + i - chip + count, count)
        return pltpu.make_async_copy(
            src.at[rel, pl.ds(0, w_rows), pl.ds(lo, width)],
            wbuf.at[pl.ds(pl.multiple_of(i * feat + spot * w_rows, 64), w_rows)],
            sem_w.at[2 * i + which],
        )

    for i in range(count):
        x_copy(i).start()
    for i in range(count):
        w_copy(i, 0).start()
        w_copy(i, 1).start()
    if has_scale:
        for i in range(count):
            x_copy(i).wait()
        scale_ref[...] = scale_in[...]
    else:
        scale_ref[...] = jnp.zeros_like(scale_ref)
        for i in range(count):
            x_copy(i).wait()

            def add_squares(r, unused):
                at_rows = pl.ds(pl.multiple_of(r * tile, tile), tile)
                total = scale_ref[at_rows]
                for g in range(feat // 128):
                    at_col = i * feat + g * 128
                    part = xbuf[at_rows, at_col : at_col + 128].astype(jnp.float32)
                    total = total + part * part
                scale_ref[at_rows] = total
                return unused

            lax.fori_loop(0, rows // tile, add_squares, 0)
        mean = jnp.sum(scale_ref[...], axis=1, keepdims=True) * (1.0 / (feat * count))
        scale_ref[...] = jnp.broadcast_to(lax.rsqrt(mean + EPSILON), scale_ref.shape)
        outs[-1][...] = scale_ref[...]

    for i in range(count):
        feature = lax.rem(tp + i, count)

        def normalize(r, unused):
            at_rows = pl.ds(pl.multiple_of(r * tile, tile), tile)
            scale = scale_ref[at_rows]
            for g in range(feat // 128):
                at_col = i * feat + g * 128
                part = xbuf[at_rows, at_col : at_col + 128].astype(jnp.float32)
                by = gain[feature, :, g * 128 : (g + 1) * 128]
                xbuf[at_rows, at_col : at_col + 128] = (part * scale * by).astype(jnp.bfloat16)
            return unused

        lax.fori_loop(0, rows // tile, normalize, 0)
    for i in range(count):
        w_copy(i, 0).wait()
        w_copy(i, 1).wait()
    acc[...] = jnp.dot(xbuf[...], wbuf[...], preferred_element_type=jnp.float32)
    cosine = cos[...]
    sine = sin[...]

    def rotated(at_col):
        head = acc[:, at_col : at_col + HD]
        return (head * cosine + pltpu.roll(head, HD // 2, 1) * sine).astype(jnp.bfloat16)

    for h in range(n_q):
        outs[0][h] = rotated(h * HD)
    if kv:
        out = outs[1 if n_q else 0]
        base = 0
        if has_old:
            base = old.shape[0]
            out[:base] = old[...]
        k_at = n_q * HD
        out[base : base + rows, :HD] = rotated(k_at)
        out[base : base + rows, HD:] = acc[:, k_at + HD : k_at + 2 * HD].astype(jnp.bfloat16)


def project(place, pieces, mine, other, gain, cos, sin, n_q, kv, lo, old=None, scale=None):
    count = len(pieces)
    rows, feat = pieces[0].shape
    width = n_q * HD + (2 * HD if kv else 0)
    outs = []
    if n_q:
        outs.append(jax.ShapeDtypeStruct((n_q, rows, HD), jnp.bfloat16))
    if kv:
        extra = old.shape[0] if old is not None else 0
        outs.append(jax.ShapeDtypeStruct((rows + extra, 2 * HD), jnp.bfloat16))
    if scale is None:
        outs.append(jax.ShapeDtypeStruct((rows, 128), jnp.float32))
    kernel = functools.partial(
        proj_kernel,
        count=count,
        rows=rows,
        feat=feat,
        width=width,
        lo=lo,
        n_q=n_q,
        kv=kv,
        has_scale=scale is not None,
        has_old=old is not None,
    )
    operands = [place, *pieces, mine, other, gain, cos, sin]
    specs = [pl.BlockSpec(memory_space=SMEM)]
    specs += [pl.BlockSpec(memory_space=pl.ANY)] * (count + 2)
    specs += [pl.BlockSpec(memory_space=VMEM)] * 3
    for more in (old, scale):
        if more is not None:
            operands.append(more)
            specs.append(pl.BlockSpec(memory_space=VMEM))
    return pl.pallas_call(
        kernel,
        out_shape=tuple(outs),
        in_specs=specs,
        out_specs=tuple(pl.BlockSpec(memory_space=VMEM) for _ in outs),
        scratch_shapes=[
            pltpu.VMEM((rows, count * feat), jnp.bfloat16),
            pltpu.VMEM((count * feat, width), jnp.bfloat16),
            pltpu.VMEM((rows, width), jnp.float32),
            pltpu.VMEM((rows, 128), jnp.float32),
            pltpu.SemaphoreType.DMA((count,)),
            pltpu.SemaphoreType.DMA((2 * count,)),
        ],
        compiler_params=pltpu.CompilerParams(vmem_limit_bytes=32 * 1024 * 1024),
        cost_estimate=pl.CostEstimate(
            flops=2 * rows * feat * count * width,
            bytes_accessed=2 * feat * count * (width + rows),
            transcendentals=0,
        ),
    )(*operands)


def attend_kernel(
    info, q_a, q_b, far, near, own, *refs, lo, hi
):
    out, qbuf, kvbuf, sbuf, mbuf, lbuf, obuf, tbuf, sems, sem_out = refs[-10:]
    heads, part, _ = q_a.shape
    tok = own.shape[0]
    local = tok // BLOCK
    back = 2 * local
    copies = [
        pltpu.make_async_copy(q_a, qbuf.at[:, pl.ds(0, part)], sems.at[0]),
        pltpu.make_async_copy(q_b, qbuf.at[:, pl.ds(part, tok - part)], sems.at[1]),
        pltpu.make_async_copy(far, kvbuf.at[pl.ds(BLOCK, tok)], sems.at[2]),
        pltpu.make_async_copy(near, kvbuf.at[pl.ds(BLOCK + tok, tok)], sems.at[3]),
        pltpu.make_async_copy(own, kvbuf.at[pl.ds(BLOCK + 2 * tok, tok)], sems.at[4]),
    ]
    for copy in copies:
        copy.start()
    kvbuf[:BLOCK] = jnp.zeros((BLOCK, 2 * HD), jnp.bfloat16)
    for copy in copies:
        copy.wait()
    first = info[0]
    n_prompts = info.shape[0] - 1
    factor = math.log2(math.e) / math.sqrt(HD)
    rows = heads * BLOCK
    row = lax.broadcasted_iota(jnp.int32, (rows, BLOCK), 0)
    col = lax.broadcasted_iota(jnp.int32, (rows, BLOCK), 1)
    causal = col <= jnp.bitwise_and(row, BLOCK - 1)

    def result_copy(i):
        at = pl.ds(pl.multiple_of(i * BLOCK, BLOCK), BLOCK)
        return pltpu.make_async_copy(tbuf.at[i - lo], out.at[at], sem_out.at[i - lo])

    def one_block(i, unused):
        block = first + i

        def find(p, state):
            start, best = state
            best = jnp.where(start <= block, start, best)
            return start + info[1 + p], best

        _, begin = lax.fori_loop(0, n_prompts, find, (jnp.int32(0), jnp.int32(0)))
        low = jnp.maximum(begin - first + back, i) + 1
        last = back + i + 1
        pairs = (last - low + 2) // 2
        q = qbuf[:, pl.ds(pl.multiple_of(i * BLOCK, BLOCK), BLOCK), :].reshape(rows, HD)

        def span(t):
            return pl.ds(pl.multiple_of((last - 1 - 2 * t) * BLOCK, BLOCK), 2 * BLOCK)

        def score(t):
            s = lax.dot_general(
                q,
                kvbuf[span(t), :HD],
                (((1,), (1,)), ((), ())),
                preferred_element_type=jnp.float32,
            )
            inside = last - 1 - 2 * t >= low
            bias = jnp.where(inside, 0.0, -1e30)
            return s[:, :BLOCK] * factor + bias, s[:, BLOCK:] * factor

        left, right = score(0)
        right = jnp.where(causal, right, -1e30)
        sbuf[0, :, :BLOCK] = left
        sbuf[0, :, BLOCK:] = right
        mbuf[...] = jnp.maximum(left, right)

        def upward(t, unused):
            left, right = score(t)
            sbuf[t, :, :BLOCK] = left
            sbuf[t, :, BLOCK:] = right
            mbuf[...] = jnp.maximum(mbuf[...], jnp.maximum(left, right))
            return unused

        lax.fori_loop(1, pairs, upward, 0)
        top = jnp.max(mbuf[...], axis=1, keepdims=True)
        mbuf[...] = jnp.broadcast_to(top, mbuf.shape)
        lbuf[...] = jnp.zeros_like(lbuf)
        obuf[...] = jnp.zeros_like(obuf)

        def gather(t, unused):
            peak = mbuf[...]
            left = jnp.exp2(sbuf[t, :, :BLOCK] - peak)
            right = jnp.exp2(sbuf[t, :, BLOCK:] - peak)
            lbuf[...] += left + right
            p = jnp.concatenate([left.astype(jnp.bfloat16), right.astype(jnp.bfloat16)], axis=1)
            obuf[...] += jnp.dot(p, kvbuf[span(t), HD:], preferred_element_type=jnp.float32)
            return unused

        lax.fori_loop(0, pairs, gather, 0)
        total = jnp.sum(lbuf[...], axis=1, keepdims=True)
        result = (obuf[...] / total).astype(jnp.bfloat16)
        for h in range(heads):
            tbuf[i - lo, :, h * HD : (h + 1) * HD] = result[h * BLOCK : (h + 1) * BLOCK]
        result_copy(i).start()
        return unused

    lax.fori_loop(lo, hi, one_block, 0)
    for i in range(lo, hi):
        result_copy(i).wait()


def attend(info, q_a, q_b, far, near, own, lo, hi, base=None):
    heads = q_a.shape[0]
    tok = own.shape[0]
    operands = [info, q_a, q_b, far, near, own]
    if base is not None:
        operands.append(base)
    return pl.pallas_call(
        functools.partial(attend_kernel, lo=lo, hi=hi),
        out_shape=jax.ShapeDtypeStruct((tok, heads * HD), jnp.bfloat16),
        in_specs=[pl.BlockSpec(memory_space=SMEM)]
        + [pl.BlockSpec(memory_space=pl.ANY)] * (len(operands) - 1),
        out_specs=pl.BlockSpec(memory_space=pl.ANY),
        scratch_shapes=[
            pltpu.VMEM((heads, tok, HD), jnp.bfloat16),
            pltpu.VMEM((3 * tok + BLOCK, 2 * HD), jnp.bfloat16),
            pltpu.VMEM(((LEN_BLOCKS + 1) // 2, heads * BLOCK, 2 * BLOCK), jnp.float32),
            pltpu.VMEM((heads * BLOCK, BLOCK), jnp.float32),
            pltpu.VMEM((heads * BLOCK, BLOCK), jnp.float32),
            pltpu.VMEM((heads * BLOCK, HD), jnp.float32),
            pltpu.VMEM((hi - lo, BLOCK, heads * HD), jnp.bfloat16),
            pltpu.SemaphoreType.DMA((5,)),
            pltpu.SemaphoreType.DMA((hi - lo,)),
        ],
        input_output_aliases={6: 0} if base is not None else {},
        compiler_params=pltpu.CompilerParams(vmem_limit_bytes=24 * 1024 * 1024),
        cost_estimate=pl.CostEstimate(
            flops=2 * 10**9 * (hi - lo), bytes_accessed=4 * 10**6, transcendentals=10**6
        ),
    )(*operands)


def cache_kernel(place, own_mine, own_other, table, mine, other, mine_mid, other_mid, out, sem, *, local, count, tok):
    chip, core, me = place[1], place[2], place[3]
    mid = count // 2
    slots = out.shape[0]

    def put(src, at_row, slot):
        return pltpu.make_async_copy(src.at[pl.ds(pl.multiple_of(at_row, BLOCK), BLOCK)], out.at[slot], sem)

    def one(b, rank):
        source = b // local
        inner = lax.rem(b, local)
        rel = lax.rem(source // 2 - chip + count, count)
        same = lax.rem(source, 2) == core
        entry = rel * local + inner
        hit = jnp.where(same, own_mine[entry], own_other[entry]) == me

        @pl.when(hit)
        def _():
            slot = table[0, rank]
            middle = rel == mid
            spot = jnp.where(rel > mid, rel - 1, jnp.where(middle, 0, rel))
            at_row = spot * tok + inner * BLOCK

            @pl.when(same & jnp.logical_not(middle))
            def _():
                put(mine, at_row, slot).start()

            @pl.when(jnp.logical_not(same) & jnp.logical_not(middle))
            def _():
                put(other, at_row, slot).start()

            @pl.when(same & middle)
            def _():
                put(mine_mid, at_row, slot).start()

            @pl.when(jnp.logical_not(same) & middle)
            def _():
                put(other_mid, at_row, slot).start()

        return rank + hit.astype(jnp.int32)

    found = lax.fori_loop(0, 2 * count * local, one, jnp.int32(0))

    def clear(r, unused):
        out[table[0, r]] = jnp.zeros(out.shape[1:], out.dtype)
        return unused

    lax.fori_loop(found, slots, clear, 0)

    def settle(r, unused):
        put(mine, 0, 0).wait()
        return unused

    lax.fori_loop(0, found, settle, 0)


def fill_cache(place, own_mine, own_other, table, mine, other, mine_mid, other_mid, local, count):
    tok = mine_mid.shape[0]
    slots = table.shape[1]
    return pl.pallas_call(
        functools.partial(cache_kernel, local=local, count=count, tok=tok),
        out_shape=jax.ShapeDtypeStruct((slots, BLOCK, mine.shape[1]), jnp.bfloat16),
        in_specs=[pl.BlockSpec(memory_space=SMEM)] * 4 + [pl.BlockSpec(memory_space=pl.ANY)] * 4,
        out_specs=pl.BlockSpec(memory_space=VMEM),
        scratch_shapes=[pltpu.SemaphoreType.DMA],
        compiler_params=pltpu.CompilerParams(vmem_limit_bytes=16 * 1024 * 1024),
    )(place, own_mine, own_other, table, mine, other, mine_mid, other_mid)


def on_device(
    hidden_states, norm_gain, w_query, w_key, w_value, prompt_blocks, owner_map, slot_table
):
    tok, feat = hidden_states.shape
    n_dev = lax.axis_size("dev")
    n_tp = lax.axis_size("tp")
    device = lax.axis_index("dev")
    count = n_dev // 2
    mid = count // 2
    local = tok // BLOCK
    heads = w_query.shape[1] // HD
    place = jnp.stack([lax.axis_index("tp"), device // 2, device % 2, device]).astype(jnp.int32)

    part = tok // 2
    x_a = ring(hidden_states[:part], "tp", 1, True)
    x_b = ring(hidden_states[part:], "tp", 1, False)

    weights = jnp.concatenate([w_query, w_key, w_value], axis=1)
    w_rows, w_cols = weights.shape
    labels = jnp.pad(owner_map.astype(jnp.bfloat16)[None], ((0, 7), (0, w_cols - local)))
    weights = jnp.concatenate([weights, labels], axis=0)
    mine = jnp.stack(ring(weights, "dev", 2, True))
    other = swap(mine, "dev")
    own_mine = mine[:, w_rows, :local].astype(jnp.int32).reshape(-1)
    own_other = other[:, w_rows, :local].astype(jnp.int32).reshape(-1)

    token_rows = device * tok + jnp.arange(tok, dtype=jnp.int32)
    starts = (jnp.cumsum(prompt_blocks) - prompt_blocks) * BLOCK
    start_of = jnp.max(jnp.where(token_rows[:, None] >= starts[None, :], starts[None, :], 0), axis=1)
    offsets = token_rows - start_of
    freq_index = jnp.arange(HD // 2, dtype=jnp.float32)
    inverse = jnp.exp(freq_index * (-2.0 * math.log(THETA) / HD))
    angles = offsets.astype(jnp.float32)[:, None] * inverse[None, :]
    cosine, sine = jnp.cos(angles), jnp.sin(angles)
    cos = jnp.concatenate([cosine, cosine], axis=1)
    sin = jnp.concatenate([-sine, sine], axis=1)
    gain = norm_gain.astype(jnp.float32).reshape(n_tp, 1, feat)

    q_width = heads * HD
    q_a, kv_a, _ = project(place, x_a, mine, other, gain, cos[:part], sin[:part], heads, True, 0)
    kv, scale_b = project(
        place, x_b, mine, other, gain, cos[part:], sin[part:], 0, True, q_width, old=kv_a
    )
    (q_b,) = project(
        place, x_b, mine, other, gain, cos[part:], sin[part:], heads, False, 0, scale=scale_b
    )

    near = lax.ppermute(kv, "dev", [(i, i + 1) for i in range(n_dev - 1)])
    k_got = ring(kv, "dev", 2, False)
    far = k_got[count - 1]
    info = jnp.concatenate([(device * local)[None].astype(jnp.int32), prompt_blocks])
    split = local // 2
    context = attend(info, q_a, q_b, far, near, kv, 0, split)
    context = attend(info, q_a, q_b, far, near, kv, split, local, base=context)
    k_mine = jnp.concatenate([k_got[i] for i in range(count) if i != mid], axis=0)
    k_other = swap(k_mine, "dev")
    k_mid_other = swap(k_got[mid], "dev")
    kv_cache = fill_cache(
        place, own_mine, own_other, slot_table, k_mine, k_other, k_got[mid], k_mid_other, local, count
    )
    return (context, kv_cache)


def solution(mesh):
    in_specs = (
        P(("groups", "dev"), "tp"),
        P(),
        P("dev", "tp"),
        P("dev", "tp"),
        P("dev", "tp"),
        P("groups"),
        P(("groups", "dev")),
        P(("groups", "dev"), None),
    )
    out_specs = (P(("groups", "dev"), "tp"), P(("groups", "dev"), None, "tp"))

    return jax.shard_map(on_device, mesh=mesh, in_specs=in_specs, out_specs=out_specs, check_vma=False)
```

```python
import functools
import math

import jax
import jax.numpy as jnp
from jax import lax
from jax.experimental import pallas as pl
from jax.experimental.pallas import tpu as pltpu
from jax.sharding import PartitionSpec as P


HD = 128
BLOCK = 128
LEN_BLOCKS = 11
EPSILON = 1e-06
THETA = 1000000.0
VMEM = pltpu.MemorySpace.VMEM
SMEM = pltpu.MemorySpace.SMEM
VMEM_ALL = 60 * 1024 * 1024
VMEM_SOME = 24 * 1024 * 1024


def ring(block, axis, hop, last_ahead):
    size = lax.axis_size(axis)
    count = size // hop
    ahead = [(i, (i + hop) % size) for i in range(size)]
    back = [(i, (i - hop) % size) for i in range(size)]
    got = {0: block}
    up = down = block
    for step in range(1, count // 2):
        up = lax.ppermute(up, axis, ahead)
        down = lax.ppermute(down, axis, back)
        got[count - step] = up
        got[step] = down
    if last_ahead:
        got[count // 2] = lax.ppermute(up, axis, ahead)
    else:
        got[count // 2] = lax.ppermute(down, axis, back)
    return [got[i] for i in range(count)]


def swap(block, axis):
    size = lax.axis_size(axis)
    return lax.ppermute(block, axis, [(i, i ^ 1) for i in range(size)])


def proj_kernel(place, *refs, count, rows, feat, width, lo, n_q, kv, has_scale, has_old):
    x_refs = refs[:count]
    mine, other, gain, cos, sin = refs[count : count + 5]
    at = count + 5
    old = scale_in = None
    if has_old:
        old = refs[at]
        at += 1
    if has_scale:
        scale_in = refs[at]
        at += 1
    n_out = (1 if n_q else 0) + (1 if kv else 0) + (0 if has_scale else 1)
    outs = refs[at : at + n_out]
    xbuf, wbuf, acc, scale_ref, sem_x, sem_w = refs[at + n_out :]
    tp, chip, core = place[0], place[1], place[2]
    w_rows = feat // 2
    tile = 64

    def x_copy(i, src):
        spot = pl.multiple_of(i * feat, 128)
        return pltpu.make_async_copy(src, xbuf.at[:, pl.ds(spot, feat)], sem_x.at[i])

    def w_copy(i, which):
        src = mine if which == 0 else other
        spot = core if which == 0 else 1 - core
        rel = jnp.bitwise_and(tp + i - chip, count - 1)
        return pltpu.make_async_copy(
            src.at[rel, pl.ds(0, w_rows), pl.ds(lo, width)],
            wbuf.at[pl.ds(pl.multiple_of(i * feat + spot * w_rows, 64), w_rows)],
            sem_w.at[2 * i + which],
        )

    for i in range(count):
        x_copy(i, x_refs[i]).start()

    def fetch(i, unused):
        w_copy(i, 0).start()
        w_copy(i, 1).start()
        return unused

    lax.fori_loop(0, count, fetch, 0)
    acc[...] = jnp.zeros_like(acc)
    if has_scale:
        scale_ref[...] = scale_in[...]
    else:
        scale_ref[...] = jnp.zeros_like(scale_ref)

        def add_piece(i, unused):
            x_copy(i, x_refs[0]).wait()

            def add_squares(r, unused):
                at_rows = pl.ds(pl.multiple_of(r * tile, tile), tile)
                total = scale_ref[at_rows]
                for g in range(feat // 128):
                    at_col = pl.ds(pl.multiple_of(i * feat + g * 128, 128), 128)
                    part = xbuf[at_rows, at_col].astype(jnp.float32)
                    total = total + part * part
                scale_ref[at_rows] = total
                return unused

            return lax.fori_loop(0, rows // tile, add_squares, unused)

        lax.fori_loop(0, count, add_piece, 0)
        mean = jnp.sum(scale_ref[...], axis=1, keepdims=True) * (1.0 / (feat * count))
        scale_ref[...] = jnp.broadcast_to(lax.rsqrt(mean + EPSILON), scale_ref.shape)
        outs[-1][...] = scale_ref[...]

    def multiply(c, unused):
        for k in range(2):
            i = 2 * c + k
            feature = jnp.bitwise_and(tp + i, count - 1)
            if has_scale:
                x_copy(i, x_refs[0]).wait()

            def normalize(r, unused):
                at_rows = pl.ds(pl.multiple_of(r * tile, tile), tile)
                scale = scale_ref[at_rows]
                for g in range(feat // 128):
                    at_col = pl.ds(pl.multiple_of(i * feat + g * 128, 128), 128)
                    part = xbuf[at_rows, at_col].astype(jnp.float32)
                    by = gain[feature, :, g * 128 : (g + 1) * 128]
                    xbuf[at_rows, at_col] = (part * scale * by).astype(jnp.bfloat16)
                return unused

            lax.fori_loop(0, rows // tile, normalize, 0)
            w_copy(i, 0).wait()
            w_copy(i, 1).wait()
        span = pl.ds(pl.multiple_of(c * 2 * feat, 256), 2 * feat)
        acc[...] += jnp.dot(xbuf[:, span], wbuf[span], preferred_element_type=jnp.float32)
        return unused

    lax.fori_loop(0, count // 2, multiply, 0)
    cosine = cos[...]
    sine = sin[...]

    def rotated(at_col):
        head = acc[:, at_col : at_col + HD]
        return (head * cosine + pltpu.roll(head, HD // 2, 1) * sine).astype(jnp.bfloat16)

    for h in range(n_q):
        outs[0][h] = rotated(h * HD)
    if kv:
        out = outs[1 if n_q else 0]
        base = 0
        if has_old:
            base = old.shape[0]
            out[:base] = old[...]
        k_at = n_q * HD
        out[base : base + rows, :HD] = rotated(k_at)
        out[base : base + rows, HD:] = acc[:, k_at + HD : k_at + 2 * HD].astype(jnp.bfloat16)


def project(place, pieces, mine, other, gain, cos, sin, n_q, kv, lo, old=None, scale=None):
    count = len(pieces)
    rows, feat = pieces[0].shape
    width = n_q * HD + (2 * HD if kv else 0)
    outs = []
    if n_q:
        outs.append(jax.ShapeDtypeStruct((n_q, rows, HD), jnp.bfloat16))
    if kv:
        extra = old.shape[0] if old is not None else 0
        outs.append(jax.ShapeDtypeStruct((rows + extra, 2 * HD), jnp.bfloat16))
    if scale is None:
        outs.append(jax.ShapeDtypeStruct((rows, 128), jnp.float32))
    kernel = functools.partial(
        proj_kernel,
        count=count,
        rows=rows,
        feat=feat,
        width=width,
        lo=lo,
        n_q=n_q,
        kv=kv,
        has_scale=scale is not None,
        has_old=old is not None,
    )
    operands = [place, *pieces, mine, other, gain, cos, sin]
    specs = [pl.BlockSpec(memory_space=SMEM)]
    specs += [pl.BlockSpec(memory_space=pl.ANY)] * (count + 2)
    specs += [pl.BlockSpec(memory_space=VMEM)] * 3
    for more in (old, scale):
        if more is not None:
            operands.append(more)
            specs.append(pl.BlockSpec(memory_space=VMEM))
    return pl.pallas_call(
        kernel,
        out_shape=tuple(outs),
        in_specs=specs,
        out_specs=tuple(pl.BlockSpec(memory_space=VMEM) for _ in outs),
        scratch_shapes=[
            pltpu.VMEM((rows, count * feat), jnp.bfloat16),
            pltpu.VMEM((count * feat, width), jnp.bfloat16),
            pltpu.VMEM((rows, width), jnp.float32),
            pltpu.VMEM((rows, 128), jnp.float32),
            pltpu.SemaphoreType.DMA((count,)),
            pltpu.SemaphoreType.DMA((2 * count,)),
        ],
        compiler_params=pltpu.CompilerParams(vmem_limit_bytes=VMEM_ALL),
        cost_estimate=pl.CostEstimate(
            flops=2 * rows * feat * count * width,
            bytes_accessed=2 * feat * count * (width + rows),
            transcendentals=0,
        ),
    )(*operands)


def attend_kernel(
    info, q_a, q_b, far, near, own, *refs, lo, hi
):
    out, qbuf, kvbuf, sbuf, mbuf, lbuf, obuf, tbuf, sems, sem_out = refs[-10:]
    heads, part, _ = q_a.shape
    tok = own.shape[0]
    local = tok // BLOCK
    back = 2 * local
    copies = [
        pltpu.make_async_copy(q_a, qbuf.at[:, pl.ds(0, part)], sems.at[0]),
        pltpu.make_async_copy(q_b, qbuf.at[:, pl.ds(part, tok - part)], sems.at[1]),
        pltpu.make_async_copy(far, kvbuf.at[pl.ds(BLOCK, tok)], sems.at[2]),
        pltpu.make_async_copy(near, kvbuf.at[pl.ds(BLOCK + tok, tok)], sems.at[3]),
        pltpu.make_async_copy(own, kvbuf.at[pl.ds(BLOCK + 2 * tok, tok)], sems.at[4]),
    ]
    for copy in copies:
        copy.start()
    kvbuf[:BLOCK] = jnp.zeros((BLOCK, 2 * HD), jnp.bfloat16)
    for copy in copies:
        copy.wait()
    first = info[0]
    n_prompts = info.shape[0] - 1
    factor = math.log2(math.e) / math.sqrt(HD)
    rows = heads * BLOCK
    row = lax.broadcasted_iota(jnp.int32, (BLOCK, BLOCK), 0)
    col = lax.broadcasted_iota(jnp.int32, (BLOCK, BLOCK), 1)
    causal = col <= row

    def result_copy(i):
        at = pl.ds(pl.multiple_of(i * BLOCK, BLOCK), BLOCK)
        return pltpu.make_async_copy(tbuf.at[i - lo], out.at[at], sem_out.at[i - lo])

    def one_block(i, unused):
        block = first + i

        def find(p, state):
            start, best = state
            best = jnp.where(start <= block, start, best)
            return start + info[1 + p], best

        _, begin = lax.fori_loop(0, n_prompts, find, (jnp.int32(0), jnp.int32(0)))
        low = jnp.maximum(begin - first + back, i) + 1
        last = back + i + 1
        pairs = (last - low + 2) // 2
        q = qbuf[:, pl.ds(pl.multiple_of(i * BLOCK, BLOCK), BLOCK), :].reshape(rows, HD)

        def span(t):
            return pl.ds(pl.multiple_of((last - 1 - 2 * t) * BLOCK, BLOCK), 2 * BLOCK)

        def score(t, h):
            s = lax.dot_general(
                q[h * BLOCK : (h + 1) * BLOCK],
                kvbuf[span(t), :HD],
                (((1,), (1,)), ((), ())),
                preferred_element_type=jnp.float32,
            )
            inside = last - 1 - 2 * t >= low
            bias = jnp.where(inside, 0.0, -1e30)
            return s[:, :BLOCK] * factor + bias, s[:, BLOCK:] * factor

        for h in range(heads):
            at = slice(h * BLOCK, (h + 1) * BLOCK)
            left, right = score(0, h)
            right = jnp.where(causal, right, -1e30)
            sbuf[0, at, :BLOCK] = left
            sbuf[0, at, BLOCK:] = right
            mbuf[at] = jnp.maximum(left, right)

        def upward(t, unused):
            for h in range(heads):
                at = slice(h * BLOCK, (h + 1) * BLOCK)
                left, right = score(t, h)
                sbuf[t, at, :BLOCK] = left
                sbuf[t, at, BLOCK:] = right
                mbuf[at] = jnp.maximum(mbuf[at], jnp.maximum(left, right))
            return unused

        lax.fori_loop(1, pairs, upward, 0)
        top = jnp.max(mbuf[...], axis=1, keepdims=True)
        mbuf[...] = jnp.broadcast_to(top, mbuf.shape)
        lbuf[...] = jnp.zeros_like(lbuf)
        obuf[...] = jnp.zeros_like(obuf)

        def gather(t, unused):
            for h in range(heads):
                at = slice(h * BLOCK, (h + 1) * BLOCK)
                peak = mbuf[at]
                left = jnp.exp2(sbuf[t, at, :BLOCK] - peak)
                right = jnp.exp2(sbuf[t, at, BLOCK:] - peak)
                lbuf[at] += left + right
                p = jnp.concatenate([left.astype(jnp.bfloat16), right.astype(jnp.bfloat16)], axis=1)
                obuf[at] += jnp.dot(p, kvbuf[span(t), HD:], preferred_element_type=jnp.float32)
            return unused

        lax.fori_loop(0, pairs, gather, 0)
        total = jnp.sum(lbuf[...], axis=1, keepdims=True)
        result = (obuf[...] / total).astype(jnp.bfloat16)
        for h in range(heads):
            tbuf[i - lo, :, h * HD : (h + 1) * HD] = result[h * BLOCK : (h + 1) * BLOCK]
        result_copy(i).start()
        return unused

    lax.fori_loop(lo, hi, one_block, 0)
    for i in range(lo, hi):
        result_copy(i).wait()


def attend(info, q_a, q_b, far, near, own, lo, hi, base=None):
    heads = q_a.shape[0]
    tok = own.shape[0]
    operands = [info, q_a, q_b, far, near, own]
    if base is not None:
        operands.append(base)
    return pl.pallas_call(
        functools.partial(attend_kernel, lo=lo, hi=hi),
        out_shape=jax.ShapeDtypeStruct((tok, heads * HD), jnp.bfloat16),
        in_specs=[pl.BlockSpec(memory_space=SMEM)]
        + [pl.BlockSpec(memory_space=pl.ANY)] * (len(operands) - 1),
        out_specs=pl.BlockSpec(memory_space=pl.ANY),
        scratch_shapes=[
            pltpu.VMEM((heads, tok, HD), jnp.bfloat16),
            pltpu.VMEM((3 * tok + BLOCK, 2 * HD), jnp.bfloat16),
            pltpu.VMEM(((LEN_BLOCKS + 1) // 2, heads * BLOCK, 2 * BLOCK), jnp.float32),
            pltpu.VMEM((heads * BLOCK, BLOCK), jnp.float32),
            pltpu.VMEM((heads * BLOCK, BLOCK), jnp.float32),
            pltpu.VMEM((heads * BLOCK, HD), jnp.float32),
            pltpu.VMEM((hi - lo, BLOCK, heads * HD), jnp.bfloat16),
            pltpu.SemaphoreType.DMA((5,)),
            pltpu.SemaphoreType.DMA((hi - lo,)),
        ],
        input_output_aliases={6: 0} if base is not None else {},
        compiler_params=pltpu.CompilerParams(vmem_limit_bytes=VMEM_SOME),
        cost_estimate=pl.CostEstimate(
            flops=2 * 10**9 * (hi - lo), bytes_accessed=4 * 10**6, transcendentals=10**6
        ),
    )(*operands)


def cache_kernel(place, own_mine, own_other, table, mine, other, mine_mid, other_mid, out, sem, *, local, count, tok):
    chip, core, me = place[1], place[2], place[3]
    mid = count // 2
    slots = out.shape[0]

    def put(src, at_row, slot):
        return pltpu.make_async_copy(src.at[pl.ds(pl.multiple_of(at_row, BLOCK), BLOCK)], out.at[slot], sem)

    def one(source, rank):
        rel = jnp.bitwise_and(jnp.right_shift(source, 1) - chip, count - 1)
        same = jnp.bitwise_and(source, 1) == core
        middle = rel == mid
        spot = jnp.where(rel > mid, rel - 1, jnp.where(middle, 0, rel))
        for inner in range(local):
            entry = rel * local + inner
            hit = jnp.where(same, own_mine[entry], own_other[entry]) == me

            @pl.when(hit)
            def _():
                slot = table[0, rank]
                at_row = spot * tok + inner * BLOCK

                @pl.when(same & jnp.logical_not(middle))
                def _():
                    put(mine, at_row, slot).start()

                @pl.when(jnp.logical_not(same) & jnp.logical_not(middle))
                def _():
                    put(other, at_row, slot).start()

                @pl.when(same & middle)
                def _():
                    put(mine_mid, at_row, slot).start()

                @pl.when(jnp.logical_not(same) & middle)
                def _():
                    put(other_mid, at_row, slot).start()

            rank = rank + hit.astype(jnp.int32)
        return rank

    found = lax.fori_loop(0, 2 * count, one, jnp.int32(0))

    def clear(r, unused):
        out[table[0, r]] = jnp.zeros(out.shape[1:], out.dtype)
        return unused

    lax.fori_loop(found, slots, clear, 0)

    def settle(r, unused):
        put(mine, 0, 0).wait()
        return unused

    lax.fori_loop(0, found, settle, 0)


def fill_cache(place, own_mine, own_other, table, mine, other, mine_mid, other_mid, local, count):
    tok = mine_mid.shape[0]
    slots = table.shape[1]
    return pl.pallas_call(
        functools.partial(cache_kernel, local=local, count=count, tok=tok),
        out_shape=jax.ShapeDtypeStruct((slots, BLOCK, mine.shape[1]), jnp.bfloat16),
        in_specs=[pl.BlockSpec(memory_space=SMEM)] * 4 + [pl.BlockSpec(memory_space=pl.ANY)] * 4,
        out_specs=pl.BlockSpec(memory_space=VMEM),
        scratch_shapes=[pltpu.SemaphoreType.DMA],
        compiler_params=pltpu.CompilerParams(vmem_limit_bytes=VMEM_SOME),
    )(place, own_mine, own_other, table, mine, other, mine_mid, other_mid)


def on_device(
    hidden_states, norm_gain, w_query, w_key, w_value, prompt_blocks, owner_map, slot_table
):
    tok, feat = hidden_states.shape
    n_dev = lax.axis_size("dev")
    n_tp = lax.axis_size("tp")
    device = lax.axis_index("dev")
    count = n_dev // 2
    assert count & (count - 1) == 0 and count == n_tp
    mid = count // 2
    local = tok // BLOCK
    heads = w_query.shape[1] // HD
    place = jnp.stack([lax.axis_index("tp"), device // 2, device % 2, device]).astype(jnp.int32)

    part = tok // 2
    x_a = ring(hidden_states[:part], "tp", 1, True)
    x_b = ring(hidden_states[part:], "tp", 1, False)

    weights = jnp.concatenate([w_query, w_key, w_value], axis=1)
    w_rows, w_cols = weights.shape
    labels = jnp.pad(owner_map.astype(jnp.bfloat16)[None], ((0, 7), (0, w_cols - local)))
    weights = jnp.concatenate([weights, labels], axis=0)
    mine = jnp.stack(ring(weights, "dev", 2, True))
    other = swap(mine, "dev")
    own_mine = mine[:, w_rows, :local].astype(jnp.int32).reshape(-1)
    own_other = other[:, w_rows, :local].astype(jnp.int32).reshape(-1)
    place, own_mine, own_other = lax.optimization_barrier((place, own_mine, own_other))

    token_rows = device * tok + jnp.arange(tok, dtype=jnp.int32)
    starts = (jnp.cumsum(prompt_blocks) - prompt_blocks) * BLOCK
    start_of = jnp.max(jnp.where(token_rows[:, None] >= starts[None, :], starts[None, :], 0), axis=1)
    offsets = token_rows - start_of
    freq_index = jnp.arange(HD // 2, dtype=jnp.float32)
    inverse = jnp.exp(freq_index * (-2.0 * math.log(THETA) / HD))
    angles = offsets.astype(jnp.float32)[:, None] * inverse[None, :]
    cosine, sine = jnp.cos(angles), jnp.sin(angles)
    cos = jnp.concatenate([cosine, cosine], axis=1)
    sin = jnp.concatenate([-sine, sine], axis=1)
    gain = norm_gain.astype(jnp.float32).reshape(n_tp, 1, feat)

    q_width = heads * HD
    q_a, kv_a, _ = project(place, x_a, mine, other, gain, cos[:part], sin[:part], heads, True, 0)
    kv, scale_b = project(
        place, x_b, mine, other, gain, cos[part:], sin[part:], 0, True, q_width, old=kv_a
    )
    (q_b,) = project(
        place, x_b, mine, other, gain, cos[part:], sin[part:], heads, False, 0, scale=scale_b
    )

    near = lax.ppermute(kv, "dev", [(i, i + 1) for i in range(n_dev - 1)])
    k_got = ring(kv, "dev", 2, False)
    far = k_got[count - 1]
    info = jnp.concatenate([(device * local)[None].astype(jnp.int32), prompt_blocks])
    cuts = (0, local // 2, local - 1, local)
    context = attend(info, q_a, q_b, far, near, kv, cuts[0], cuts[1])
    context = attend(info, q_a, q_b, far, near, kv, cuts[1], cuts[2], base=context)
    context = attend(info, q_a, q_b, far, near, kv, cuts[2], cuts[3], base=context)
    k_mine = jnp.concatenate([k_got[i] for i in range(count) if i != mid], axis=0)
    k_other = swap(k_mine, "dev")
    k_mid_other = swap(k_got[mid], "dev")
    kv_cache = fill_cache(
        place, own_mine, own_other, slot_table, k_mine, k_other, k_got[mid], k_mid_other, local, count
    )
    return (context, kv_cache)


def solution(mesh):
    in_specs = (
        P(("groups", "dev"), "tp"),
        P(),
        P("dev", "tp"),
        P("dev", "tp"),
        P("dev", "tp"),
        P("groups"),
        P(("groups", "dev")),
        P(("groups", "dev"), None),
    )
    out_specs = (P(("groups", "dev"), "tp"), P(("groups", "dev"), None, "tp"))

    return jax.shard_map(on_device, mesh=mesh, in_specs=in_specs, out_specs=out_specs, check_vma=False)
```

```python
import functools
import math

import jax
import jax.numpy as jnp
from jax import lax
from jax.experimental import pallas as pl
from jax.experimental.pallas import tpu as pltpu
from jax.sharding import PartitionSpec as P


HD = 128
BLOCK = 128
LEN_BLOCKS = 11
EPSILON = 1e-06
THETA = 1000000.0
VMEM = pltpu.MemorySpace.VMEM
SMEM = pltpu.MemorySpace.SMEM
VMEM_ALL = 60 * 1024 * 1024
VMEM_SOME = 24 * 1024 * 1024


def ring(block, axis, hop, last_ahead):
    size = lax.axis_size(axis)
    count = size // hop
    ahead = [(i, (i + hop) % size) for i in range(size)]
    back = [(i, (i - hop) % size) for i in range(size)]
    got = {0: block}
    up = down = block
    for step in range(1, count // 2):
        up = lax.ppermute(up, axis, ahead)
        down = lax.ppermute(down, axis, back)
        got[count - step] = up
        got[step] = down
    if last_ahead:
        got[count // 2] = lax.ppermute(up, axis, ahead)
    else:
        got[count // 2] = lax.ppermute(down, axis, back)
    return [got[i] for i in range(count)]


def swap(block, axis):
    size = lax.axis_size(axis)
    return lax.ppermute(block, axis, [(i, i ^ 1) for i in range(size)])


def proj_kernel(place, *refs, count, rows, feat, width, lo, n_q, kv, normed, hand_on, has_old):
    n_x = 1 if normed else count
    x_refs = refs[:n_x]
    mine, other, mine_mid, other_mid, gain, cos, sin = refs[n_x : n_x + 7]
    at = n_x + 7
    old = None
    if has_old:
        old = refs[at]
        at += 1
    n_out = (1 if n_q else 0) + (1 if kv else 0) + (1 if hand_on else 0)
    outs = refs[at : at + n_out]
    xbuf, wbuf, acc, scale_ref, sem_x, sem_w, sem_out = refs[at + n_out :]
    tp, chip, core = place[0], place[1], place[2]
    w_rows = feat // 2
    mid = count // 2
    tile = 64

    def x_copy(i):
        if normed:
            return pltpu.make_async_copy(x_refs[0], xbuf, sem_x.at[0])
        return pltpu.make_async_copy(x_refs[i], xbuf.at[:, pl.ds(i * feat, feat)], sem_x.at[i])

    def w_copy(rel, which):
        spot = core if which == 0 else 1 - core
        if rel == mid:
            src = mine_mid if which == 0 else other_mid
        else:
            src = (mine if which == 0 else other).at[rel if rel < mid else rel - 1]
        i = jnp.bitwise_and(chip + rel - tp, count - 1)
        return pltpu.make_async_copy(
            src.at[pl.ds(0, w_rows), pl.ds(lo, width)],
            wbuf.at[pl.ds(pl.multiple_of(i * feat + spot * w_rows, 64), w_rows)],
            sem_w.at[2 * rel + which],
        )

    for i in range(n_x):
        x_copy(i).start()
    for rel in range(count):
        w_copy(rel, 0).start()
        w_copy(rel, 1).start()
    for i in range(n_x):
        x_copy(i).wait()
    hand = None
    if not normed:

        def add_squares(r, unused):
            at_rows = pl.ds(pl.multiple_of(r * tile, tile), tile)
            totals = [jnp.zeros((tile, 128), jnp.float32) for _ in range(2)]
            for g in range(count * feat // 128):
                part = xbuf[at_rows, g * 128 : (g + 1) * 128].astype(jnp.float32)
                totals[g % 2] = totals[g % 2] + part * part
            scale_ref[at_rows] = totals[0] + totals[1]
            return unused

        lax.fori_loop(0, rows // tile, add_squares, 0)
        mean = jnp.sum(scale_ref[...], axis=1, keepdims=True) * (1.0 / (feat * count))
        scale_ref[...] = jnp.broadcast_to(lax.rsqrt(mean + EPSILON), scale_ref.shape)

        def normalize(r, unused):
            at_rows = pl.ds(pl.multiple_of(r * tile, tile), tile)
            scale = scale_ref[at_rows]
            for g in range(count * feat // 128):
                at_col = slice(g * 128, (g + 1) * 128)
                part = xbuf[at_rows, at_col].astype(jnp.float32)
                xbuf[at_rows, at_col] = (part * scale * gain[:, at_col]).astype(jnp.bfloat16)
            return unused

        lax.fori_loop(0, rows // tile, normalize, 0)
    for rel in range(count):
        w_copy(rel, 0).wait()
        w_copy(rel, 1).wait()
    acc[...] = jnp.dot(xbuf[...], wbuf[...], preferred_element_type=jnp.float32)
    if hand_on:
        hand = pltpu.make_async_copy(xbuf, outs[-1], sem_out)
        hand.start()
    cosine = cos[...]
    sine = sin[...]

    def rotated(at_col):
        head = acc[:, at_col : at_col + HD]
        return (head * cosine + pltpu.roll(head, HD // 2, 1) * sine).astype(jnp.bfloat16)

    for h in range(n_q):
        outs[0][h] = rotated(h * HD)
    if kv:
        out = outs[1 if n_q else 0]
        base = 0
        if has_old:
            base = old.shape[0]
            out[:base] = old[...]
        k_at = n_q * HD
        out[base : base + rows, :HD] = rotated(k_at)
        out[base : base + rows, HD:] = acc[:, k_at + HD : k_at + 2 * HD].astype(jnp.bfloat16)
    if hand_on:
        hand.wait()


def project(place, pieces, weights, gain, cos, sin, n_q, kv, lo, old=None, hand_on=False):
    normed = len(pieces) == 1
    count = weights[0].shape[0] + 1
    rows = pieces[0].shape[0]
    feat = pieces[0].shape[1] // (count if normed else 1)
    width = n_q * HD + (2 * HD if kv else 0)
    outs = []
    out_specs = []
    if n_q:
        outs.append(jax.ShapeDtypeStruct((n_q, rows, HD), jnp.bfloat16))
        out_specs.append(pl.BlockSpec(memory_space=VMEM))
    if kv:
        extra = old.shape[0] if old is not None else 0
        outs.append(jax.ShapeDtypeStruct((rows + extra, 2 * HD), jnp.bfloat16))
        out_specs.append(pl.BlockSpec(memory_space=VMEM))
    if hand_on:
        outs.append(jax.ShapeDtypeStruct((rows, count * feat), jnp.bfloat16))
        out_specs.append(pl.BlockSpec(memory_space=pl.ANY))
    kernel = functools.partial(
        proj_kernel,
        count=count,
        rows=rows,
        feat=feat,
        width=width,
        lo=lo,
        n_q=n_q,
        kv=kv,
        normed=normed,
        hand_on=hand_on,
        has_old=old is not None,
    )
    operands = [place, *pieces, *weights, gain, cos, sin]
    specs = [pl.BlockSpec(memory_space=SMEM)]
    specs += [pl.BlockSpec(memory_space=pl.ANY)] * (len(pieces) + 4)
    specs += [pl.BlockSpec(memory_space=VMEM)] * 3
    if old is not None:
        operands.append(old)
        specs.append(pl.BlockSpec(memory_space=VMEM))
    return pl.pallas_call(
        kernel,
        out_shape=tuple(outs),
        in_specs=specs,
        out_specs=tuple(out_specs),
        scratch_shapes=[
            pltpu.VMEM((rows, count * feat), jnp.bfloat16),
            pltpu.VMEM((count * feat, width), jnp.bfloat16),
            pltpu.VMEM((rows, width), jnp.float32),
            pltpu.VMEM((rows, 128), jnp.float32),
            pltpu.SemaphoreType.DMA((len(pieces),)),
            pltpu.SemaphoreType.DMA((2 * count,)),
            pltpu.SemaphoreType.DMA,
        ],
        compiler_params=pltpu.CompilerParams(vmem_limit_bytes=VMEM_ALL),
        cost_estimate=pl.CostEstimate(
            flops=2 * rows * feat * count * width,
            bytes_accessed=2 * feat * count * (width + rows),
            transcendentals=0,
        ),
    )(*operands)


def attend_kernel(
    info, q_a, q_b, far, near, own, *refs, lo, hi
):
    out, qbuf, kvbuf, sbuf, mbuf, lbuf, obuf, tbuf, sems, sem_out = refs[-10:]
    heads, part, _ = q_a.shape
    tok = own.shape[0]
    local = tok // BLOCK
    back = 2 * local
    copies = [
        pltpu.make_async_copy(q_a, qbuf.at[:, pl.ds(0, part)], sems.at[0]),
        pltpu.make_async_copy(q_b, qbuf.at[:, pl.ds(part, tok - part)], sems.at[1]),
        pltpu.make_async_copy(far, kvbuf.at[pl.ds(BLOCK, tok)], sems.at[2]),
        pltpu.make_async_copy(near, kvbuf.at[pl.ds(BLOCK + tok, tok)], sems.at[3]),
        pltpu.make_async_copy(own, kvbuf.at[pl.ds(BLOCK + 2 * tok, tok)], sems.at[4]),
    ]
    for copy in copies:
        copy.start()
    kvbuf[:BLOCK] = jnp.zeros((BLOCK, 2 * HD), jnp.bfloat16)
    for copy in copies:
        copy.wait()
    first = info[0]
    n_prompts = info.shape[0] - 1
    factor = math.log2(math.e) / math.sqrt(HD)
    rows = heads * BLOCK
    row = lax.broadcasted_iota(jnp.int32, (BLOCK, BLOCK), 0)
    col = lax.broadcasted_iota(jnp.int32, (BLOCK, BLOCK), 1)
    causal = col <= row

    def result_copy(i):
        at = pl.ds(pl.multiple_of(i * BLOCK, BLOCK), BLOCK)
        return pltpu.make_async_copy(tbuf.at[i - lo], out.at[at], sem_out.at[i - lo])

    def one_block(i, unused):
        block = first + i

        def find(p, state):
            start, best = state
            best = jnp.where(start <= block, start, best)
            return start + info[1 + p], best

        _, begin = lax.fori_loop(0, n_prompts, find, (jnp.int32(0), jnp.int32(0)))
        low = jnp.maximum(begin - first + back, i) + 1
        last = back + i + 1
        pairs = (last - low + 2) // 2
        q = qbuf[:, pl.ds(pl.multiple_of(i * BLOCK, BLOCK), BLOCK), :].reshape(rows, HD)

        def span(t):
            return pl.ds(pl.multiple_of((last - 1 - 2 * t) * BLOCK, BLOCK), 2 * BLOCK)

        def score(t, h):
            s = lax.dot_general(
                q[h * BLOCK : (h + 1) * BLOCK],
                kvbuf[span(t), :HD],
                (((1,), (1,)), ((), ())),
                preferred_element_type=jnp.float32,
            )
            inside = last - 1 - 2 * t >= low
            bias = jnp.where(inside, 0.0, -1e30)
            return s[:, :BLOCK] * factor + bias, s[:, BLOCK:] * factor

        mbuf[...] = jnp.full_like(mbuf, -1e30)

        def upward(t, unused):
            shut = jnp.where(t == 0, -1e30, 0.0)
            for h in range(heads):
                at = slice(h * BLOCK, (h + 1) * BLOCK)
                left, right = score(t, h)
                right = right + jnp.where(causal, 0.0, shut)
                sbuf[t, at, :BLOCK] = left
                sbuf[t, at, BLOCK:] = right
                mbuf[at] = jnp.maximum(mbuf[at], jnp.maximum(left, right))
            return unused

        lax.fori_loop(0, pairs, upward, 0)
        top = jnp.max(mbuf[...], axis=1, keepdims=True)
        mbuf[...] = jnp.broadcast_to(top, mbuf.shape)
        lbuf[...] = jnp.zeros_like(lbuf)
        obuf[...] = jnp.zeros_like(obuf)

        def gather(t, unused):
            for h in range(heads):
                at = slice(h * BLOCK, (h + 1) * BLOCK)
                peak = mbuf[at]
                left = jnp.exp2(sbuf[t, at, :BLOCK] - peak)
                right = jnp.exp2(sbuf[t, at, BLOCK:] - peak)
                lbuf[at] += left + right
                p = jnp.concatenate([left.astype(jnp.bfloat16), right.astype(jnp.bfloat16)], axis=1)
                obuf[at] += jnp.dot(p, kvbuf[span(t), HD:], preferred_element_type=jnp.float32)
            return unused

        lax.fori_loop(0, pairs, gather, 0)
        total = jnp.sum(lbuf[...], axis=1, keepdims=True)
        result = (obuf[...] / total).astype(jnp.bfloat16)
        for h in range(heads):
            tbuf[i - lo, :, h * HD : (h + 1) * HD] = result[h * BLOCK : (h + 1) * BLOCK]
        result_copy(i).start()
        return unused

    lax.fori_loop(lo, hi, one_block, 0)
    for i in range(lo, hi):
        result_copy(i).wait()


def attend(info, q_a, q_b, far, near, own, lo, hi, base=None):
    heads = q_a.shape[0]
    tok = own.shape[0]
    operands = [info, q_a, q_b, far, near, own]
    if base is not None:
        operands.append(base)
    return pl.pallas_call(
        functools.partial(attend_kernel, lo=lo, hi=hi),
        out_shape=jax.ShapeDtypeStruct((tok, heads * HD), jnp.bfloat16),
        in_specs=[pl.BlockSpec(memory_space=SMEM)]
        + [pl.BlockSpec(memory_space=pl.ANY)] * (len(operands) - 1),
        out_specs=pl.BlockSpec(memory_space=pl.ANY),
        scratch_shapes=[
            pltpu.VMEM((heads, tok, HD), jnp.bfloat16),
            pltpu.VMEM((3 * tok + BLOCK, 2 * HD), jnp.bfloat16),
            pltpu.VMEM(((LEN_BLOCKS + 1) // 2, heads * BLOCK, 2 * BLOCK), jnp.float32),
            pltpu.VMEM((heads * BLOCK, BLOCK), jnp.float32),
            pltpu.VMEM((heads * BLOCK, BLOCK), jnp.float32),
            pltpu.VMEM((heads * BLOCK, HD), jnp.float32),
            pltpu.VMEM((hi - lo, BLOCK, heads * HD), jnp.bfloat16),
            pltpu.SemaphoreType.DMA((5,)),
            pltpu.SemaphoreType.DMA((hi - lo,)),
        ],
        input_output_aliases={6: 0} if base is not None else {},
        compiler_params=pltpu.CompilerParams(vmem_limit_bytes=VMEM_SOME),
        cost_estimate=pl.CostEstimate(
            flops=2 * 10**9 * (hi - lo), bytes_accessed=4 * 10**6, transcendentals=10**6
        ),
    )(*operands)


def cache_kernel(place, own_mine, own_other, table, mine, other, mine_mid, other_mid, out, sem, *, local, count, tok):
    chip, core, me = place[1], place[2], place[3]
    mid = count // 2
    slots = out.shape[0]

    def put(src, at_row, slot):
        return pltpu.make_async_copy(src.at[pl.ds(pl.multiple_of(at_row, BLOCK), BLOCK)], out.at[slot], sem)

    def one(source, rank):
        rel = jnp.bitwise_and(jnp.right_shift(source, 1) - chip, count - 1)
        same = jnp.bitwise_and(source, 1) == core
        middle = rel == mid
        spot = jnp.where(rel > mid, rel - 1, jnp.where(middle, 0, rel))
        for inner in range(local):
            entry = rel * local + inner
            hit = jnp.where(same, own_mine[entry], own_other[entry]) == me

            @pl.when(hit)
            def _():
                slot = table[0, rank]
                at_row = spot * tok + inner * BLOCK

                @pl.when(same & jnp.logical_not(middle))
                def _():
                    put(mine, at_row, slot).start()

                @pl.when(jnp.logical_not(same) & jnp.logical_not(middle))
                def _():
                    put(other, at_row, slot).start()

                @pl.when(same & middle)
                def _():
                    put(mine_mid, at_row, slot).start()

                @pl.when(jnp.logical_not(same) & middle)
                def _():
                    put(other_mid, at_row, slot).start()

            rank = rank + hit.astype(jnp.int32)
        return rank

    found = lax.fori_loop(0, 2 * count, one, jnp.int32(0))

    def clear(r, unused):
        out[table[0, r]] = jnp.zeros(out.shape[1:], out.dtype)
        return unused

    lax.fori_loop(found, slots, clear, 0)

    def settle(r, unused):
        put(mine, 0, 0).wait()
        return unused

    lax.fori_loop(0, found, settle, 0)


def fill_cache(place, own_mine, own_other, table, mine, other, mine_mid, other_mid, local, count):
    tok = mine_mid.shape[0]
    slots = table.shape[1]
    return pl.pallas_call(
        functools.partial(cache_kernel, local=local, count=count, tok=tok),
        out_shape=jax.ShapeDtypeStruct((slots, BLOCK, mine.shape[1]), jnp.bfloat16),
        in_specs=[pl.BlockSpec(memory_space=SMEM)] * 4 + [pl.BlockSpec(memory_space=pl.ANY)] * 4,
        out_specs=pl.BlockSpec(memory_space=VMEM),
        scratch_shapes=[pltpu.SemaphoreType.DMA],
        compiler_params=pltpu.CompilerParams(vmem_limit_bytes=VMEM_SOME),
    )(place, own_mine, own_other, table, mine, other, mine_mid, other_mid)


def on_device(
    hidden_states, norm_gain, w_query, w_key, w_value, prompt_blocks, owner_map, slot_table
):
    tok, feat = hidden_states.shape
    n_dev = lax.axis_size("dev")
    n_tp = lax.axis_size("tp")
    device = lax.axis_index("dev")
    count = n_dev // 2
    assert count & (count - 1) == 0 and count == n_tp
    mid = count // 2
    local = tok // BLOCK
    heads = w_query.shape[1] // HD
    place = jnp.stack([lax.axis_index("tp"), device // 2, device % 2, device]).astype(jnp.int32)

    part = tok // 2
    x_a = ring(hidden_states[:part], "tp", 1, True)
    x_b = ring(hidden_states[part:], "tp", 1, False)

    weights = jnp.concatenate([w_query, w_key, w_value], axis=1)
    w_rows, w_cols = weights.shape
    labels = jnp.pad(owner_map.astype(jnp.bfloat16)[None], ((0, 7), (0, w_cols - local)))
    weights = jnp.concatenate([weights, labels], axis=0)
    w_got = ring(weights, "dev", 2, True)
    w_mine = jnp.stack([w_got[i] for i in range(count) if i != mid])
    w_other = swap(w_mine, "dev")
    w_other_mid = swap(w_got[mid], "dev")
    w_set = (w_mine, w_other, w_got[mid], w_other_mid)

    def labels_of(most, middle):
        by_rel = jnp.concatenate(
            [most[:mid, w_rows, :local], middle[w_rows : w_rows + 1, :local], most[mid:, w_rows, :local]]
        )
        return by_rel.astype(jnp.int32).reshape(-1)

    own_mine, own_other = labels_of(w_mine, w_got[mid]), labels_of(w_other, w_other_mid)
    place, own_mine, own_other = lax.optimization_barrier((place, own_mine, own_other))

    token_rows = device * tok + jnp.arange(tok, dtype=jnp.int32)
    starts = (jnp.cumsum(prompt_blocks) - prompt_blocks) * BLOCK
    start_of = jnp.max(jnp.where(token_rows[:, None] >= starts[None, :], starts[None, :], 0), axis=1)
    offsets = token_rows - start_of
    freq_index = jnp.arange(HD // 2, dtype=jnp.float32)
    inverse = jnp.exp(freq_index * (-2.0 * math.log(THETA) / HD))
    angles = offsets.astype(jnp.float32)[:, None] * inverse[None, :]
    cosine, sine = jnp.cos(angles), jnp.sin(angles)
    cos = jnp.concatenate([cosine, cosine], axis=1)
    sin = jnp.concatenate([-sine, sine], axis=1)
    gain = norm_gain.astype(jnp.float32).reshape(n_tp, feat)
    turn = lax.rem(lax.axis_index("tp") + jnp.arange(n_tp), n_tp)
    gain = jnp.take(gain, turn, axis=0, mode="clip").reshape(1, n_tp * feat)

    q_width = heads * HD
    q_a, kv_a = project(place, x_a, w_set, gain, cos[:part], sin[:part], heads, True, 0)
    kv, normed_b = project(
        place, x_b, w_set, gain, cos[part:], sin[part:], 0, True, q_width, kv_a, True
    )
    (q_b,) = project(place, [normed_b], w_set, gain, cos[part:], sin[part:], heads, False, 0)

    near = lax.ppermute(kv, "dev", [(i, i + 1) for i in range(n_dev - 1)])
    k_got = ring(kv, "dev", 2, False)
    far = k_got[count - 1]
    info = jnp.concatenate([(device * local)[None].astype(jnp.int32), prompt_blocks])
    cuts = (0, local // 2, local - 1, local)
    context = attend(info, q_a, q_b, far, near, kv, cuts[0], cuts[1])
    context = attend(info, q_a, q_b, far, near, kv, cuts[1], cuts[2], base=context)
    context = attend(info, q_a, q_b, far, near, kv, cuts[2], cuts[3], base=context)
    k_mine = jnp.concatenate([k_got[i] for i in range(count) if i != mid], axis=0)
    k_other = swap(k_mine, "dev")
    k_mid_other = swap(k_got[mid], "dev")
    kv_cache = fill_cache(
        place, own_mine, own_other, slot_table, k_mine, k_other, k_got[mid], k_mid_other, local, count
    )
    return (context, kv_cache)


def solution(mesh):
    in_specs = (
        P(("groups", "dev"), "tp"),
        P(),
        P("dev", "tp"),
        P("dev", "tp"),
        P("dev", "tp"),
        P("groups"),
        P(("groups", "dev")),
        P(("groups", "dev"), None),
    )
    out_specs = (P(("groups", "dev"), "tp"), P(("groups", "dev"), None, "tp"))

    return jax.shard_map(on_device, mesh=mesh, in_specs=in_specs, out_specs=out_specs, check_vma=False)
```

```python
import functools
import math

import jax
import jax.numpy as jnp
from jax import lax
from jax.experimental import pallas as pl
from jax.experimental.pallas import tpu as pltpu
from jax.sharding import PartitionSpec as P


HD = 128
BLOCK = 128
LEN_BLOCKS = 11
EPSILON = 1e-06
THETA = 1000000.0
VMEM = pltpu.MemorySpace.VMEM
SMEM = pltpu.MemorySpace.SMEM
MIB = 1024 * 1024


def ring(block, axis, hop, last_ahead, tied=None):
    size = lax.axis_size(axis)
    count = size // hop
    ahead = [(i, (i + hop) % size) for i in range(size)]
    back = [(i, (i - hop) % size) for i in range(size)]
    got = {0: block}
    up = down = block
    for step in range(1, count // 2):
        up = lax.ppermute(up, axis, ahead)
        down = lax.ppermute(down, axis, back)
        got[count - step] = up
        got[step] = down
        if tied and step == 1:
            up, *tied[:] = lax.optimization_barrier((up, *tied))
    if last_ahead:
        got[count // 2] = lax.ppermute(up, axis, ahead)
    else:
        got[count // 2] = lax.ppermute(down, axis, back)
    return [got[i] for i in range(count)]


def swap(block, axis):
    size = lax.axis_size(axis)
    return lax.ppermute(block, axis, [(i, i ^ 1) for i in range(size)])


def by_arrival(count):
    order = [0]
    for step in range(1, count // 2):
        order += [step, count - step]
    return order


def weight_copies(place, weights, wbuf, sem, count, feat, lo, width):
    tp, chip, core = place[0], place[1], place[2]
    mine, other, mine_mid, other_mid = weights
    w_rows = feat // 2
    copies = []
    for k, rel in enumerate([*by_arrival(count), count // 2]):
        i = jnp.bitwise_and(chip + rel - tp, count - 1)
        for which in range(2):
            spot = core if which == 0 else 1 - core
            if rel == count // 2:
                src = mine_mid if which == 0 else other_mid
            else:
                src = (mine if which == 0 else other).at[k]
            copies.append(
                pltpu.make_async_copy(
                    src.at[pl.ds(0, w_rows), pl.ds(lo, width)],
                    wbuf.at[pl.ds(pl.multiple_of(i * feat + spot * w_rows, 64), w_rows)],
                    sem.at[2 * rel + which],
                )
            )
    return copies


def rotated(head, cos, sin):
    return (head * cos[...] + pltpu.roll(head, HD // 2, 1) * sin[...]).astype(jnp.bfloat16)


def keys_kernel(place, *refs, count, part, feat, lo):
    pieces = refs[: 2 * count]
    weights = refs[2 * count : 2 * count + 4]
    gain, cos, sin, kv, labels, normed = refs[2 * count + 4 : 2 * count + 10]
    xbuf, wbuf, acc, tags, sem_x, sem_w, sem_tag, sem_out = refs[2 * count + 10 :]
    w_rows = feat // 2
    tile = 64
    mid = count // 2

    def x_copy(half, i):
        return pltpu.make_async_copy(
            pieces[half * count + i],
            xbuf.at[pl.ds(half * part, part), pl.ds(i * feat, feat)],
            sem_x.at[half * count + i],
        )

    def tag_copies():
        copies = []
        for which in range(2):
            for k, rel in enumerate([*by_arrival(count), mid]):
                src = weights[2 + which] if rel == mid else weights[which].at[k]
                copies.append(
                    pltpu.make_async_copy(
                        src.at[pl.ds(w_rows, 8), pl.ds(0, 128)],
                        tags.at[which * count + rel],
                        sem_tag.at[which * count + rel],
                    )
                )
        return copies

    w_copies = weight_copies(place, weights, wbuf, sem_w, count, feat, lo, 2 * HD)
    t_copies = tag_copies()
    for i in range(count):
        x_copy(0, i).start()
    for i in range(count):
        x_copy(1, i).start()
    for copy in w_copies + t_copies:
        copy.start()

    def normalize(r, unused):
        at_rows = pl.ds(pl.multiple_of(r * tile, tile), tile)
        totals = [jnp.zeros((tile, 128), jnp.float32) for _ in range(2)]
        for g in range(count * feat // 128):
            part_x = xbuf[at_rows, g * 128 : (g + 1) * 128].astype(jnp.float32)
            totals[g % 2] = totals[g % 2] + part_x * part_x
        mean = jnp.sum(totals[0] + totals[1], axis=1, keepdims=True) * (1.0 / (feat * count))
        scale = jnp.broadcast_to(lax.rsqrt(mean + EPSILON), (tile, 128))
        for g in range(count * feat // 128):
            at_col = slice(g * 128, (g + 1) * 128)
            part_x = xbuf[at_rows, at_col].astype(jnp.float32)
            xbuf[at_rows, at_col] = (part_x * scale * gain[:, at_col]).astype(jnp.bfloat16)
        return unused

    handed = []
    for half in range(2):
        for i in range(count):
            x_copy(half, i).wait()
        lax.fori_loop(half * part // tile, (half + 1) * part // tile, normalize, 0)
        rows = pl.ds(half * part, part)
        handed.append(pltpu.make_async_copy(xbuf.at[rows], normed.at[rows], sem_out.at[half]))
        handed[-1].start()
    for copy in w_copies:
        copy.wait()
    acc[...] = jnp.dot(xbuf[...], wbuf[...], preferred_element_type=jnp.float32)
    kv[:, :HD] = rotated(acc[:, :HD], cos, sin)
    kv[:, HD:] = acc[:, HD:].astype(jnp.bfloat16)
    for copy in t_copies:
        copy.wait()
    for r in range(2 * count):
        labels[r : r + 1, :] = tags[r].astype(jnp.float32)[0:1].astype(jnp.int32)
    for copy in handed:
        copy.wait()


def queries_kernel(place, x, mine, other, mine_mid, other_mid, cos, sin, q, xbuf, wbuf, acc, sem_x, sem_w, *, count, part, feat, heads):
    def x_copy(half):
        rows = pl.ds(half * part, part)
        return pltpu.make_async_copy(x.at[rows], xbuf.at[rows], sem_x.at[half])

    weights = (mine, other, mine_mid, other_mid)
    w_copies = weight_copies(place, weights, wbuf, sem_w, count, feat, 0, heads * HD)
    for copy in w_copies:
        copy.start()
    for half in range(2):
        x_copy(half).start()
    for copy in w_copies:
        copy.wait()

    def one_half(half, unused):
        x_copy(half).wait()
        rows = pl.ds(pl.multiple_of(half * part, 64), part)
        acc[...] = jnp.dot(xbuf[rows], wbuf[...], preferred_element_type=jnp.float32)
        for h in range(heads):
            q[h, rows] = rotated(acc[:, h * HD : (h + 1) * HD], cos.at[rows], sin.at[rows])
        return unused

    lax.fori_loop(0, 2, one_half, 0)


def project_keys(place, pieces, weights, gain, cos, sin, lo):
    count = len(pieces) // 2
    part, feat = pieces[0].shape
    tok = 2 * part
    return pl.pallas_call(
        functools.partial(keys_kernel, count=count, part=part, feat=feat, lo=lo),
        out_shape=(
            jax.ShapeDtypeStruct((tok, 2 * HD), jnp.bfloat16),
            jax.ShapeDtypeStruct((2 * count, 128), jnp.int32),
            jax.ShapeDtypeStruct((tok, count * feat), jnp.bfloat16),
        ),
        in_specs=[pl.BlockSpec(memory_space=SMEM)]
        + [pl.BlockSpec(memory_space=pl.ANY)] * (len(pieces) + 4)
        + [pl.BlockSpec(memory_space=VMEM)] * 3,
        out_specs=(
            pl.BlockSpec(memory_space=VMEM),
            pl.BlockSpec(memory_space=VMEM),
            pl.BlockSpec(memory_space=pl.ANY),
        ),
        scratch_shapes=[
            pltpu.VMEM((tok, count * feat), jnp.bfloat16),
            pltpu.VMEM((count * feat, 2 * HD), jnp.bfloat16),
            pltpu.VMEM((tok, 2 * HD), jnp.float32),
            pltpu.VMEM((2 * count, 8, 128), jnp.bfloat16),
            pltpu.SemaphoreType.DMA((2 * count,)),
            pltpu.SemaphoreType.DMA((2 * count,)),
            pltpu.SemaphoreType.DMA((2 * count,)),
            pltpu.SemaphoreType.DMA((2,)),
        ],
        compiler_params=pltpu.CompilerParams(vmem_limit_bytes=16 * MIB),
        cost_estimate=pl.CostEstimate(
            flops=4 * tok * feat * count * HD, bytes_accessed=4 * tok * feat * count, transcendentals=0
        ),
    )(place, *pieces, *weights, gain, cos, sin)


def project_queries(place, normed, weights, cos, sin, heads):
    count = weights[0].shape[0] + 1
    tok = normed.shape[0]
    part = tok // 2
    feat = normed.shape[1] // count
    width = heads * HD
    return pl.pallas_call(
        functools.partial(queries_kernel, count=count, part=part, feat=feat, heads=heads),
        out_shape=jax.ShapeDtypeStruct((heads, tok, HD), jnp.bfloat16),
        in_specs=[pl.BlockSpec(memory_space=SMEM)]
        + [pl.BlockSpec(memory_space=pl.ANY)] * 5
        + [pl.BlockSpec(memory_space=VMEM)] * 2,
        out_specs=pl.BlockSpec(memory_space=VMEM),
        scratch_shapes=[
            pltpu.VMEM((tok, count * feat), jnp.bfloat16),
            pltpu.VMEM((count * feat, width), jnp.bfloat16),
            pltpu.VMEM((part, width), jnp.float32),
            pltpu.SemaphoreType.DMA((2,)),
            pltpu.SemaphoreType.DMA((2 * count,)),
        ],
        compiler_params=pltpu.CompilerParams(vmem_limit_bytes=20 * MIB),
        cost_estimate=pl.CostEstimate(
            flops=2 * tok * feat * count * width, bytes_accessed=2 * tok * feat * count, transcendentals=0
        ),
    )(place, normed, *weights, cos, sin)


def attend_kernel(
    info, q_in, far, near, own, *refs, lo, hi
):
    out, qbuf, kvbuf, sbuf, mbuf, lbuf, obuf, tbuf, sems, sem_out = refs[-10:]
    heads = q_in.shape[0]
    tok = own.shape[0]
    local = tok // BLOCK
    back = 2 * local
    span_in = pl.ds(lo * BLOCK, (hi - lo) * BLOCK)
    copies = [
        pltpu.make_async_copy(q_in.at[:, span_in], qbuf.at[:, span_in], sems.at[0]),
        pltpu.make_async_copy(far, kvbuf.at[pl.ds(BLOCK, tok)], sems.at[1]),
        pltpu.make_async_copy(near, kvbuf.at[pl.ds(BLOCK + tok, tok)], sems.at[2]),
        pltpu.make_async_copy(own, kvbuf.at[pl.ds(BLOCK + 2 * tok, tok)], sems.at[3]),
    ]
    for copy in copies:
        copy.start()
    kvbuf[:BLOCK] = jnp.zeros((BLOCK, 2 * HD), jnp.bfloat16)
    for copy in copies:
        copy.wait()
    first = info[0]
    n_prompts = info.shape[0] - 1
    factor = math.log2(math.e) / math.sqrt(HD)
    rows = heads * BLOCK
    row = lax.broadcasted_iota(jnp.int32, (BLOCK, BLOCK), 0)
    col = lax.broadcasted_iota(jnp.int32, (BLOCK, BLOCK), 1)
    causal = col <= row

    def result_copy(i):
        at = pl.ds(pl.multiple_of(i * BLOCK, BLOCK), BLOCK)
        return pltpu.make_async_copy(tbuf.at[i - lo], out.at[at], sem_out.at[i - lo])

    def one_block(i, unused):
        block = first + i

        def find(p, state):
            start, best = state
            best = jnp.where(start <= block, start, best)
            return start + info[1 + p], best

        _, begin = lax.fori_loop(0, n_prompts, find, (jnp.int32(0), jnp.int32(0)))
        low = jnp.maximum(begin - first + back, i) + 1
        last = back + i + 1
        pairs = (last - low + 2) // 2
        q = qbuf[:, pl.ds(pl.multiple_of(i * BLOCK, BLOCK), BLOCK), :].reshape(rows, HD)

        def span(t):
            return pl.ds(pl.multiple_of((last - 1 - 2 * t) * BLOCK, BLOCK), 2 * BLOCK)

        def score(t, h):
            s = lax.dot_general(
                q[h * BLOCK : (h + 1) * BLOCK],
                kvbuf[span(t), :HD],
                (((1,), (1,)), ((), ())),
                preferred_element_type=jnp.float32,
            )
            inside = last - 1 - 2 * t >= low
            bias = jnp.where(inside, 0.0, -1e30)
            return s[:, :BLOCK] * factor + bias, s[:, BLOCK:] * factor

        mbuf[...] = jnp.full_like(mbuf, -1e30)

        def upward(t, unused):
            shut = jnp.where(t == 0, -1e30, 0.0)
            for h in range(heads):
                at = slice(h * BLOCK, (h + 1) * BLOCK)
                left, right = score(t, h)
                right = right + jnp.where(causal, 0.0, shut)
                sbuf[t, at, :BLOCK] = left
                sbuf[t, at, BLOCK:] = right
                mbuf[at] = jnp.maximum(mbuf[at], jnp.maximum(left, right))
            return unused

        lax.fori_loop(0, pairs, upward, 0)
        top = jnp.max(mbuf[...], axis=1, keepdims=True)
        mbuf[...] = jnp.broadcast_to(top, mbuf.shape)
        lbuf[...] = jnp.zeros_like(lbuf)
        obuf[...] = jnp.zeros_like(obuf)

        def gather(t, unused):
            for h in range(heads):
                at = slice(h * BLOCK, (h + 1) * BLOCK)
                peak = mbuf[at]
                left = jnp.exp2(sbuf[t, at, :BLOCK] - peak)
                right = jnp.exp2(sbuf[t, at, BLOCK:] - peak)
                lbuf[at] += left + right
                p = jnp.concatenate([left.astype(jnp.bfloat16), right.astype(jnp.bfloat16)], axis=1)
                obuf[at] += jnp.dot(p, kvbuf[span(t), HD:], preferred_element_type=jnp.float32)
            return unused

        lax.fori_loop(0, pairs, gather, 0)
        total = jnp.sum(lbuf[...], axis=1, keepdims=True)
        result = (obuf[...] / total).astype(jnp.bfloat16)
        for h in range(heads):
            tbuf[i - lo, :, h * HD : (h + 1) * HD] = result[h * BLOCK : (h + 1) * BLOCK]
        result_copy(i).start()
        return unused

    lax.fori_loop(lo, hi, one_block, 0)
    for i in range(lo, hi):
        result_copy(i).wait()


def attend(info, q, far, near, own, lo, hi, base=None):
    heads = q.shape[0]
    tok = own.shape[0]
    operands = [info, q, far, near, own]
    if base is not None:
        operands.append(base)
    return pl.pallas_call(
        functools.partial(attend_kernel, lo=lo, hi=hi),
        out_shape=jax.ShapeDtypeStruct((tok, heads * HD), jnp.bfloat16),
        in_specs=[pl.BlockSpec(memory_space=SMEM)]
        + [pl.BlockSpec(memory_space=pl.ANY)] * (len(operands) - 1),
        out_specs=pl.BlockSpec(memory_space=pl.ANY),
        scratch_shapes=[
            pltpu.VMEM((heads, tok, HD), jnp.bfloat16),
            pltpu.VMEM((3 * tok + BLOCK, 2 * HD), jnp.bfloat16),
            pltpu.VMEM(((LEN_BLOCKS + 1) // 2, heads * BLOCK, 2 * BLOCK), jnp.float32),
            pltpu.VMEM((heads * BLOCK, BLOCK), jnp.float32),
            pltpu.VMEM((heads * BLOCK, BLOCK), jnp.float32),
            pltpu.VMEM((heads * BLOCK, HD), jnp.float32),
            pltpu.VMEM((hi - lo, BLOCK, heads * HD), jnp.bfloat16),
            pltpu.SemaphoreType.DMA((4,)),
            pltpu.SemaphoreType.DMA((hi - lo,)),
        ],
        input_output_aliases={5: 0} if base is not None else {},
        compiler_params=pltpu.CompilerParams(vmem_limit_bytes=12 * MIB),
        cost_estimate=pl.CostEstimate(
            flops=2 * 10**9 * (hi - lo), bytes_accessed=4 * 10**6, transcendentals=10**6
        ),
    )(*operands)


def cache_kernel(place, labels, table, mine, other, mine_mid, other_mid, out, sem, *, local, count, tok):
    chip, core, me = place[1], place[2], place[3]
    mid = count // 2
    slots = out.shape[0]

    def put(src, at_row, slot):
        return pltpu.make_async_copy(src.at[pl.ds(pl.multiple_of(at_row, BLOCK), BLOCK)], out.at[slot], sem)

    def one(source, rank):
        rel = jnp.bitwise_and(jnp.right_shift(source, 1) - chip, count - 1)
        same = jnp.bitwise_and(source, 1) == core
        middle = rel == mid
        spot = jnp.where(rel > mid, 2 * (count - rel), jnp.where(middle, 0, jnp.maximum(2 * rel - 1, 0)))
        label_row = jnp.where(same, rel, count + rel)
        for inner in range(local):
            hit = labels[label_row, inner] == me

            @pl.when(hit)
            def _():
                slot = table[0, rank]
                at_row = spot * tok + inner * BLOCK

                @pl.when(same & jnp.logical_not(middle))
                def _():
                    put(mine, at_row, slot).start()

                @pl.when(jnp.logical_not(same) & jnp.logical_not(middle))
                def _():
                    put(other, at_row, slot).start()

                @pl.when(same & middle)
                def _():
                    put(mine_mid, at_row, slot).start()

                @pl.when(jnp.logical_not(same) & middle)
                def _():
                    put(other_mid, at_row, slot).start()

            rank = rank + hit.astype(jnp.int32)
        return rank

    found = lax.fori_loop(0, 2 * count, one, jnp.int32(0))

    def clear(r, unused):
        out[table[0, r]] = jnp.zeros(out.shape[1:], out.dtype)
        return unused

    lax.fori_loop(found, slots, clear, 0)

    def settle(r, unused):
        put(mine, 0, 0).wait()
        return unused

    lax.fori_loop(0, found, settle, 0)


def fill_cache(place, labels, table, mine, other, mine_mid, other_mid, local, count):
    tok = mine_mid.shape[0]
    slots = table.shape[1]
    return pl.pallas_call(
        functools.partial(cache_kernel, local=local, count=count, tok=tok),
        out_shape=jax.ShapeDtypeStruct((slots, BLOCK, mine.shape[1]), jnp.bfloat16),
        in_specs=[pl.BlockSpec(memory_space=SMEM)] * 3 + [pl.BlockSpec(memory_space=pl.ANY)] * 4,
        out_specs=pl.BlockSpec(memory_space=VMEM),
        scratch_shapes=[pltpu.SemaphoreType.DMA],
        compiler_params=pltpu.CompilerParams(vmem_limit_bytes=8 * MIB),
    )(place, labels, table, mine, other, mine_mid, other_mid)


def on_device(
    hidden_states, norm_gain, w_query, w_key, w_value, prompt_blocks, owner_map, slot_table
):
    tok, feat = hidden_states.shape
    n_dev = lax.axis_size("dev")
    n_tp = lax.axis_size("tp")
    device = lax.axis_index("dev")
    count = n_dev // 2
    assert count & (count - 1) == 0 and count == n_tp
    mid = count // 2
    local = tok // BLOCK
    heads = w_query.shape[1] // HD
    place = jnp.stack([lax.axis_index("tp"), device // 2, device % 2, device]).astype(jnp.int32)

    token_rows = device * tok + jnp.arange(tok, dtype=jnp.int32)
    starts = (jnp.cumsum(prompt_blocks) - prompt_blocks) * BLOCK
    start_of = jnp.max(jnp.where(token_rows[:, None] >= starts[None, :], starts[None, :], 0), axis=1)
    offsets = token_rows - start_of
    freq_index = jnp.arange(HD // 2, dtype=jnp.float32)
    inverse = jnp.exp(freq_index * (-2.0 * math.log(THETA) / HD))
    angles = offsets.astype(jnp.float32)[:, None] * inverse[None, :]
    cosine, sine = jnp.cos(angles), jnp.sin(angles)
    cos = jnp.concatenate([cosine, cosine], axis=1)
    sin = jnp.concatenate([-sine, sine], axis=1)
    gain = norm_gain.astype(jnp.float32)
    gain = lax.dynamic_slice_in_dim(
        jnp.concatenate([gain, gain]), lax.axis_index("tp") * feat, n_tp * feat
    )[None]
    info = jnp.concatenate([(device * local)[None].astype(jnp.int32), prompt_blocks])

    part = tok // 2
    tied = [cos, sin, gain, place, info]
    x_a = ring(hidden_states[:part], "tp", 1, True)
    x_b = ring(hidden_states[part:], "tp", 1, False, tied)
    cos, sin, gain, place, info = tied

    weights = jnp.concatenate([w_query, w_key, w_value], axis=1)
    w_cols = weights.shape[1]
    labels = jnp.pad(owner_map.astype(jnp.bfloat16)[None], ((0, 7), (0, w_cols - local)))
    weights = jnp.concatenate([weights, labels], axis=0)
    arrival = by_arrival(count)
    w_got = ring(weights, "dev", 2, True)
    w_mine = jnp.stack([w_got[i] for i in arrival])
    w_other = swap(w_mine, "dev")
    w_other_mid = swap(w_got[mid], "dev")
    w_set = (w_mine, w_other, w_got[mid], w_other_mid)

    kv, labels, normed = project_keys(place, [*x_a, *x_b], w_set, gain, cos, sin, heads * HD)
    q = project_queries(place, normed, w_set, cos, sin, heads)

    near = lax.ppermute(kv, "dev", [(i, i + 1) for i in range(n_dev - 1)])
    k_got = ring(kv, "dev", 2, False)
    far = k_got[count - 1]
    cuts = (0, local // 2, local - 1, local)
    context = attend(info, q, far, near, kv, cuts[0], cuts[1])
    context = attend(info, q, far, near, kv, cuts[1], cuts[2], base=context)
    context = attend(info, q, far, near, kv, cuts[2], cuts[3], base=context)
    k_mine = jnp.concatenate([k_got[i] for i in arrival], axis=0)
    k_other = swap(k_mine, "dev")
    k_mid_other = swap(k_got[mid], "dev")
    kv_cache = fill_cache(
        place, labels, slot_table, k_mine, k_other, k_got[mid], k_mid_other, local, count
    )
    return (context, kv_cache)


def solution(mesh):
    in_specs = (
        P(("groups", "dev"), "tp"),
        P(),
        P("dev", "tp"),
        P("dev", "tp"),
        P("dev", "tp"),
        P("groups"),
        P(("groups", "dev")),
        P(("groups", "dev"), None),
    )
    out_specs = (P(("groups", "dev"), "tp"), P(("groups", "dev"), None, "tp"))

    return jax.shard_map(on_device, mesh=mesh, in_specs=in_specs, out_specs=out_specs, check_vma=False)
```

```python
import functools
import math

import jax
import jax.numpy as jnp
from jax import lax
from jax.experimental import pallas as pl
from jax.experimental.pallas import tpu as pltpu
from jax.sharding import PartitionSpec as P


HD = 128
BLOCK = 128
LEN_BLOCKS = 11
EPSILON = 1e-06
THETA = 1000000.0
HBM = pltpu.MemorySpace.HBM
VMEM = pltpu.MemorySpace.VMEM
SMEM = pltpu.MemorySpace.SMEM
MIB = 1024 * 1024


def ring(block, axis, hop, last_ahead, tied=None):
    size = lax.axis_size(axis)
    count = size // hop
    ahead = [(i, (i + hop) % size) for i in range(size)]
    back = [(i, (i - hop) % size) for i in range(size)]
    got = {0: block}
    up = down = block
    for step in range(1, count // 2):
        up = lax.ppermute(up, axis, ahead)
        down = lax.ppermute(down, axis, back)
        got[count - step] = up
        got[step] = down
        if tied and step == 1:
            up, *tied[:] = lax.optimization_barrier((up, *tied))
    if last_ahead is None:
        half = block.shape[0] // 2
        top = lax.ppermute(up[:half], axis, ahead)
        bottom = lax.ppermute(down[half:], axis, back)
        got[count // 2] = jnp.concatenate([top, bottom], axis=0)
    elif last_ahead:
        got[count // 2] = lax.ppermute(up, axis, ahead)
    else:
        got[count // 2] = lax.ppermute(down, axis, back)
    return [got[i] for i in range(count)]


def swap(block, axis):
    size = lax.axis_size(axis)
    return lax.ppermute(block, axis, [(i, i ^ 1) for i in range(size)])


def by_arrival(count):
    order = [0]
    for step in range(1, count // 2):
        order += [step, count - step]
    return order


def weight_copies(place, weights, wbuf, sem, count, feat, lo, width):
    tp, chip, core = place[0], place[1], place[2]
    mine, other, mine_mid, other_mid = weights
    w_rows = feat // 2
    copies = []
    for k, rel in enumerate([*by_arrival(count), count // 2]):
        i = jnp.bitwise_and(chip + rel - tp, count - 1)
        for which in range(2):
            spot = core if which == 0 else 1 - core
            if rel == count // 2:
                src = mine_mid if which == 0 else other_mid
            else:
                src = (mine if which == 0 else other).at[k]
            copies.append(
                pltpu.make_async_copy(
                    src.at[pl.ds(0, w_rows), pl.ds(lo, width)],
                    wbuf.at[pl.ds(pl.multiple_of(i * feat + spot * w_rows, 64), w_rows)],
                    sem.at[2 * rel + which],
                )
            )
    return copies


def rotated(head, cos, sin):
    return (head * cos[...] + pltpu.roll(head, HD // 2, 1) * sin[...]).astype(jnp.bfloat16)


def normalize(pieces, gain, out):
    rows, feat = pieces[0].shape
    tile = 32

    def one_tile(r, unused):
        at_rows = pl.ds(pl.multiple_of(r * tile, tile), tile)
        totals = [jnp.zeros((tile, 128), jnp.float32) for _ in range(2)]
        for piece in pieces:
            for g in range(feat // 128):
                part = piece[at_rows, g * 128 : (g + 1) * 128].astype(jnp.float32)
                totals[g % 2] = totals[g % 2] + part * part
        mean = jnp.sum(totals[0] + totals[1], axis=1, keepdims=True) * (1.0 / (feat * len(pieces)))
        scale = jnp.broadcast_to(lax.rsqrt(mean + EPSILON), (tile, 128))
        for i, piece in enumerate(pieces):
            for g in range(feat // 128):
                part = piece[at_rows, g * 128 : (g + 1) * 128].astype(jnp.float32)
                at_col = slice(i * feat + g * 128, i * feat + (g + 1) * 128)
                out[at_rows, at_col] = (part * scale * gain[:, at_col]).astype(jnp.bfloat16)
        return unused

    lax.fori_loop(0, rows // tile, one_tile, 0)


def norm_kernel(*refs):
    normalize(refs[:-2], refs[-2], refs[-1])


def norm_rows(pieces, gain):
    count = len(pieces)
    rows, feat = pieces[0].shape
    return pl.pallas_call(
        norm_kernel,
        out_shape=jax.ShapeDtypeStruct((rows, count * feat), jnp.bfloat16),
        in_specs=[pl.BlockSpec(memory_space=VMEM)] * (count + 1),
        out_specs=pl.BlockSpec(memory_space=VMEM),
        compiler_params=pltpu.CompilerParams(vmem_limit_bytes=12 * MIB),
        cost_estimate=pl.CostEstimate(
            flops=6 * rows * feat * count, bytes_accessed=4 * rows * feat * count, transcendentals=0
        ),
    )(*pieces, gain)


def keys_kernel(place, x_a, *refs, count, feat, lo):
    pieces = refs[:count]
    weights = refs[count : count + 4]
    gain, cos, sin, kv, labels, x_b = refs[count + 4 : count + 10]
    wbuf, acc, tags, sem_w, sem_tag = refs[count + 10 :]
    w_rows = feat // 2
    mid = count // 2
    part = x_a.shape[0]
    w_copies = weight_copies(place, weights, wbuf, sem_w, count, feat, lo, 2 * HD)
    t_copies = []
    for which in range(2):
        for k, rel in enumerate([*by_arrival(count), mid]):
            src = weights[2 + which] if rel == mid else weights[which].at[k]
            t_copies.append(
                pltpu.make_async_copy(
                    src.at[pl.ds(w_rows, 8), pl.ds(0, 128)],
                    tags.at[which * count + rel],
                    sem_tag.at[which * count + rel],
                )
            )
    for copy in w_copies + t_copies:
        copy.start()
    normalize(pieces, gain, x_b)
    for copy in w_copies + t_copies:
        copy.wait()
    acc[:part] = jnp.dot(x_a[...], wbuf[...], preferred_element_type=jnp.float32)
    acc[part:] = jnp.dot(x_b[...], wbuf[...], preferred_element_type=jnp.float32)
    kv[:, :HD] = rotated(acc[:, :HD], cos, sin)
    kv[:, HD:] = acc[:, HD:].astype(jnp.bfloat16)
    for r in range(2 * count):
        labels[r : r + 1, :] = tags[r].astype(jnp.float32)[0:1].astype(jnp.int32)


def queries_kernel(place, x_a, x_b, mine, other, mine_mid, other_mid, cos, sin, q, wbuf, acc, sem_w, *, count, feat, heads):
    part = x_a.shape[0]
    weights = (mine, other, mine_mid, other_mid)
    w_copies = weight_copies(place, weights, wbuf, sem_w, count, feat, 0, heads * HD)
    for copy in w_copies:
        copy.start()
    for copy in w_copies:
        copy.wait()
    for half, x in enumerate((x_a, x_b)):
        rows = pl.ds(half * part, part)
        acc[...] = jnp.dot(x[...], wbuf[...], preferred_element_type=jnp.float32)
        for h in range(heads):
            q[h, rows] = rotated(acc[:, h * HD : (h + 1) * HD], cos.at[rows], sin.at[rows])


def project_keys(place, x_a, pieces, weights, gain, cos, sin, lo):
    count = len(pieces)
    part, feat = pieces[0].shape
    tok = 2 * part
    return pl.pallas_call(
        functools.partial(keys_kernel, count=count, feat=feat, lo=lo),
        out_shape=(
            jax.ShapeDtypeStruct((tok, 2 * HD), jnp.bfloat16),
            jax.ShapeDtypeStruct((2 * count, 128), jnp.int32),
            jax.ShapeDtypeStruct((part, count * feat), jnp.bfloat16),
        ),
        in_specs=[pl.BlockSpec(memory_space=SMEM)]
        + [pl.BlockSpec(memory_space=VMEM)] * (count + 1)
        + [pl.BlockSpec(memory_space=HBM)]
        + [pl.BlockSpec(memory_space=pl.ANY)] * 3
        + [pl.BlockSpec(memory_space=VMEM)] * 3,
        out_specs=(pl.BlockSpec(memory_space=VMEM),) * 3,
        scratch_shapes=[
            pltpu.VMEM((count * feat, 2 * HD), jnp.bfloat16),
            pltpu.VMEM((tok, 2 * HD), jnp.float32),
            pltpu.VMEM((2 * count, 8, 128), jnp.bfloat16),
            pltpu.SemaphoreType.DMA((2 * count,)),
            pltpu.SemaphoreType.DMA((2 * count,)),
        ],
        compiler_params=pltpu.CompilerParams(vmem_limit_bytes=20 * MIB),
        cost_estimate=pl.CostEstimate(
            flops=4 * tok * feat * count * HD, bytes_accessed=4 * tok * feat * count, transcendentals=0
        ),
    )(place, x_a, *pieces, *weights, gain, cos, sin)


def project_queries(place, x_a, x_b, weights, cos, sin, heads):
    count = weights[0].shape[0] + 1
    part = x_a.shape[0]
    tok = 2 * part
    feat = x_a.shape[1] // count
    width = heads * HD
    return pl.pallas_call(
        functools.partial(queries_kernel, count=count, feat=feat, heads=heads),
        out_shape=jax.ShapeDtypeStruct((heads, tok, HD), jnp.bfloat16),
        in_specs=[pl.BlockSpec(memory_space=SMEM)]
        + [pl.BlockSpec(memory_space=VMEM)] * 2
        + [pl.BlockSpec(memory_space=HBM)]
        + [pl.BlockSpec(memory_space=pl.ANY)] * 3
        + [pl.BlockSpec(memory_space=VMEM)] * 2,
        out_specs=pl.BlockSpec(memory_space=VMEM),
        scratch_shapes=[
            pltpu.VMEM((count * feat, width), jnp.bfloat16),
            pltpu.VMEM((part, width), jnp.float32),
            pltpu.SemaphoreType.DMA((2 * count,)),
        ],
        compiler_params=pltpu.CompilerParams(vmem_limit_bytes=20 * MIB),
        cost_estimate=pl.CostEstimate(
            flops=2 * tok * feat * count * width, bytes_accessed=2 * tok * feat * count, transcendentals=0
        ),
    )(place, x_a, x_b, *weights, cos, sin)


def attend_kernel(
    info, q_in, far, near, own, *refs, lo, hi
):
    out, qbuf, kvbuf, sbuf, mbuf, lbuf, obuf, tbuf, sems, sem_out = refs[-10:]
    heads = q_in.shape[0]
    tok = own.shape[0]
    local = tok // BLOCK
    back = 2 * local
    span_in = pl.ds(lo * BLOCK, (hi - lo) * BLOCK)
    copies = [
        pltpu.make_async_copy(q_in.at[:, span_in], qbuf.at[:, span_in], sems.at[0]),
        pltpu.make_async_copy(far, kvbuf.at[pl.ds(BLOCK, tok)], sems.at[1]),
        pltpu.make_async_copy(near, kvbuf.at[pl.ds(BLOCK + tok, tok)], sems.at[2]),
        pltpu.make_async_copy(own, kvbuf.at[pl.ds(BLOCK + 2 * tok, tok)], sems.at[3]),
    ]
    for copy in copies:
        copy.start()
    kvbuf[:BLOCK] = jnp.zeros((BLOCK, 2 * HD), jnp.bfloat16)
    for copy in copies:
        copy.wait()
    first = info[0]
    n_prompts = info.shape[0] - 1
    factor = math.log2(math.e) / math.sqrt(HD)
    rows = heads * BLOCK
    row = lax.broadcasted_iota(jnp.int32, (BLOCK, BLOCK), 0)
    col = lax.broadcasted_iota(jnp.int32, (BLOCK, BLOCK), 1)
    causal = col <= row

    def result_copy(i):
        at = pl.ds(pl.multiple_of(i * BLOCK, BLOCK), BLOCK)
        return pltpu.make_async_copy(tbuf.at[i - lo], out.at[at], sem_out.at[i - lo])

    def one_block(i, unused):
        block = first + i

        def find(p, state):
            start, best = state
            best = jnp.where(start <= block, start, best)
            return start + info[1 + p], best

        _, begin = lax.fori_loop(0, n_prompts, find, (jnp.int32(0), jnp.int32(0)))
        low = jnp.maximum(begin - first + back, i) + 1
        last = back + i + 1
        pairs = (last - low + 2) // 2
        q = qbuf[:, pl.ds(pl.multiple_of(i * BLOCK, BLOCK), BLOCK), :].reshape(rows, HD)

        def span(t):
            return pl.ds(pl.multiple_of((last - 1 - 2 * t) * BLOCK, BLOCK), 2 * BLOCK)

        def score(t, h):
            s = lax.dot_general(
                q[h * BLOCK : (h + 1) * BLOCK],
                kvbuf[span(t), :HD],
                (((1,), (1,)), ((), ())),
                preferred_element_type=jnp.float32,
            )
            inside = last - 1 - 2 * t >= low
            bias = jnp.where(inside, 0.0, -1e30)
            return s[:, :BLOCK] * factor + bias, s[:, BLOCK:] * factor

        mbuf[...] = jnp.full_like(mbuf, -1e30)

        def upward(t, unused):
            shut = jnp.where(t == 0, -1e30, 0.0)
            for h in range(heads):
                at = slice(h * BLOCK, (h + 1) * BLOCK)
                left, right = score(t, h)
                right = right + jnp.where(causal, 0.0, shut)
                sbuf[t, at, :BLOCK] = left
                sbuf[t, at, BLOCK:] = right
                mbuf[at] = jnp.maximum(mbuf[at], jnp.maximum(left, right))
            return unused

        lax.fori_loop(0, pairs, upward, 0)
        top = jnp.max(mbuf[...], axis=1, keepdims=True)
        mbuf[...] = jnp.broadcast_to(top, mbuf.shape)
        lbuf[...] = jnp.zeros_like(lbuf)
        obuf[...] = jnp.zeros_like(obuf)

        def gather(t, unused):
            for h in range(heads):
                at = slice(h * BLOCK, (h + 1) * BLOCK)
                peak = mbuf[at]
                left = jnp.exp2(sbuf[t, at, :BLOCK] - peak)
                right = jnp.exp2(sbuf[t, at, BLOCK:] - peak)
                lbuf[at] += left + right
                p = jnp.concatenate([left.astype(jnp.bfloat16), right.astype(jnp.bfloat16)], axis=1)
                obuf[at] += jnp.dot(p, kvbuf[span(t), HD:], preferred_element_type=jnp.float32)
            return unused

        lax.fori_loop(0, pairs, gather, 0)
        total = jnp.sum(lbuf[...], axis=1, keepdims=True)
        result = (obuf[...] / total).astype(jnp.bfloat16)
        for h in range(heads):
            tbuf[i - lo, :, h * HD : (h + 1) * HD] = result[h * BLOCK : (h + 1) * BLOCK]
        result_copy(i).start()
        return unused

    lax.fori_loop(lo, hi, one_block, 0)
    for i in range(lo, hi):
        result_copy(i).wait()


def attend(info, q, far, near, own, lo, hi, base=None):
    heads = q.shape[0]
    tok = own.shape[0]
    operands = [info, q, far, near, own]
    if base is not None:
        operands.append(base)
    return pl.pallas_call(
        functools.partial(attend_kernel, lo=lo, hi=hi),
        out_shape=jax.ShapeDtypeStruct((tok, heads * HD), jnp.bfloat16),
        in_specs=[pl.BlockSpec(memory_space=SMEM)]
        + [pl.BlockSpec(memory_space=pl.ANY)] * (len(operands) - 1),
        out_specs=pl.BlockSpec(memory_space=pl.ANY),
        scratch_shapes=[
            pltpu.VMEM((heads, tok, HD), jnp.bfloat16),
            pltpu.VMEM((3 * tok + BLOCK, 2 * HD), jnp.bfloat16),
            pltpu.VMEM(((LEN_BLOCKS + 1) // 2, heads * BLOCK, 2 * BLOCK), jnp.float32),
            pltpu.VMEM((heads * BLOCK, BLOCK), jnp.float32),
            pltpu.VMEM((heads * BLOCK, BLOCK), jnp.float32),
            pltpu.VMEM((heads * BLOCK, HD), jnp.float32),
            pltpu.VMEM((hi - lo, BLOCK, heads * HD), jnp.bfloat16),
            pltpu.SemaphoreType.DMA((4,)),
            pltpu.SemaphoreType.DMA((hi - lo,)),
        ],
        input_output_aliases={5: 0} if base is not None else {},
        compiler_params=pltpu.CompilerParams(vmem_limit_bytes=12 * MIB),
        cost_estimate=pl.CostEstimate(
            flops=2 * 10**9 * (hi - lo), bytes_accessed=4 * 10**6, transcendentals=10**6
        ),
    )(*operands)


def cache_kernel(place, labels, table, mine, other, mine_mid, other_mid, out, sem, *, local, count, tok):
    chip, core, me = place[1], place[2], place[3]
    mid = count // 2
    slots = out.shape[0]

    def put(src, at_row, slot):
        return pltpu.make_async_copy(src.at[pl.ds(pl.multiple_of(at_row, BLOCK), BLOCK)], out.at[slot], sem)

    def one(source, rank):
        rel = jnp.bitwise_and(jnp.right_shift(source, 1) - chip, count - 1)
        same = jnp.bitwise_and(source, 1) == core
        middle = rel == mid
        spot = jnp.where(rel > mid, 2 * (count - rel), jnp.where(middle, 0, jnp.maximum(2 * rel - 1, 0)))
        label_row = jnp.where(same, rel, count + rel)
        for inner in range(local):
            hit = labels[label_row, inner] == me

            @pl.when(hit)
            def _():
                slot = table[0, rank]
                at_row = spot * tok + inner * BLOCK

                @pl.when(same & jnp.logical_not(middle))
                def _():
                    put(mine, at_row, slot).start()

                @pl.when(jnp.logical_not(same) & jnp.logical_not(middle))
                def _():
                    put(other, at_row, slot).start()

                @pl.when(same & middle)
                def _():
                    put(mine_mid, at_row, slot).start()

                @pl.when(jnp.logical_not(same) & middle)
                def _():
                    put(other_mid, at_row, slot).start()

            rank = rank + hit.astype(jnp.int32)
        return rank

    found = lax.fori_loop(0, 2 * count, one, jnp.int32(0))

    def clear(r, unused):
        out[table[0, r]] = jnp.zeros(out.shape[1:], out.dtype)
        return unused

    lax.fori_loop(found, slots, clear, 0)

    def settle(r, unused):
        put(mine, 0, 0).wait()
        return unused

    lax.fori_loop(0, found, settle, 0)


def fill_cache(place, labels, table, mine, other, mine_mid, other_mid, local, count):
    tok = mine_mid.shape[0]
    slots = table.shape[1]
    return pl.pallas_call(
        functools.partial(cache_kernel, local=local, count=count, tok=tok),
        out_shape=jax.ShapeDtypeStruct((slots, BLOCK, mine.shape[1]), jnp.bfloat16),
        in_specs=[pl.BlockSpec(memory_space=SMEM)] * 3 + [pl.BlockSpec(memory_space=pl.ANY)] * 4,
        out_specs=pl.BlockSpec(memory_space=VMEM),
        scratch_shapes=[pltpu.SemaphoreType.DMA],
        compiler_params=pltpu.CompilerParams(vmem_limit_bytes=8 * MIB),
    )(place, labels, table, mine, other, mine_mid, other_mid)


def on_device(
    hidden_states, norm_gain, w_query, w_key, w_value, prompt_blocks, owner_map, slot_table
):
    tok, feat = hidden_states.shape
    n_dev = lax.axis_size("dev")
    n_tp = lax.axis_size("tp")
    device = lax.axis_index("dev")
    count = n_dev // 2
    assert count & (count - 1) == 0 and count == n_tp
    mid = count // 2
    local = tok // BLOCK
    heads = w_query.shape[1] // HD
    place = jnp.stack([lax.axis_index("tp"), device // 2, device % 2, device]).astype(jnp.int32)

    token_rows = device * tok + jnp.arange(tok, dtype=jnp.int32)
    starts = (jnp.cumsum(prompt_blocks) - prompt_blocks) * BLOCK
    start_of = jnp.max(jnp.where(token_rows[:, None] >= starts[None, :], starts[None, :], 0), axis=1)
    offsets = token_rows - start_of
    lane = jnp.arange(HD, dtype=jnp.int32)
    freq_index = lax.rem(lane, HD // 2).astype(jnp.float32)
    inverse = jnp.exp(freq_index * (-2.0 * math.log(THETA) / HD))
    angles = offsets.astype(jnp.float32)[:, None] * inverse[None, :]
    cos = jnp.cos(angles)
    sin = jnp.sin(angles) * jnp.where(lane < HD // 2, -1.0, 1.0)[None, :]
    gain = norm_gain.astype(jnp.float32)
    gain = lax.dynamic_slice_in_dim(
        jnp.concatenate([gain, gain]), lax.axis_index("tp") * feat, n_tp * feat
    )[None]
    info = jnp.concatenate([(device * local)[None].astype(jnp.int32), prompt_blocks])

    part = tok // 2
    tied = [cos, sin, gain, place, info]
    x_a = ring(hidden_states[:part], "tp", 1, True)
    x_b = ring(hidden_states[part:], "tp", 1, False, tied)
    cos, sin, gain, place, info = tied

    weights = jnp.concatenate([w_query, w_key, w_value], axis=1)
    w_cols = weights.shape[1]
    labels = jnp.pad(owner_map.astype(jnp.bfloat16)[None], ((0, 7), (0, w_cols - local)))
    weights = jnp.concatenate([weights, labels], axis=0)
    arrival = by_arrival(count)
    w_got = ring(weights, "dev", 2, True)
    w_mine = jnp.stack([w_got[i] for i in arrival])
    w_other = swap(w_mine, "dev")
    w_other_mid = swap(w_got[mid], "dev")
    w_set = (w_mine, w_other, w_got[mid], w_other_mid)

    n_a = norm_rows(x_a, gain)
    kv, labels, n_b = project_keys(place, n_a, x_b, w_set, gain, cos, sin, heads * HD)
    q = project_queries(place, n_a, n_b, w_set, cos, sin, heads)

    k_got = ring(kv, "dev", 2, None)
    far = k_got[count - 1]
    near = swap(jnp.where(device % 2 == 0, kv, far), "dev")
    cuts = (0, local // 2, local - 1, local)
    context = attend(info, q, far, near, kv, cuts[0], cuts[1])
    context = attend(info, q, far, near, kv, cuts[1], cuts[2], base=context)
    context = attend(info, q, far, near, kv, cuts[2], cuts[3], base=context)
    k_mine = jnp.concatenate([k_got[i] for i in arrival], axis=0)
    k_other = swap(k_mine, "dev")
    k_mid_other = swap(k_got[mid], "dev")
    kv_cache = fill_cache(
        place, labels, slot_table, k_mine, k_other, k_got[mid], k_mid_other, local, count
    )
    return (context, kv_cache)


def solution(mesh):
    in_specs = (
        P(("groups", "dev"), "tp"),
        P(),
        P("dev", "tp"),
        P("dev", "tp"),
        P("dev", "tp"),
        P("groups"),
        P(("groups", "dev")),
        P(("groups", "dev"), None),
    )
    out_specs = (P(("groups", "dev"), "tp"), P(("groups", "dev"), None, "tp"))

    return jax.shard_map(on_device, mesh=mesh, in_specs=in_specs, out_specs=out_specs, check_vma=False)
```

```python
import functools
import math

import jax
import jax.numpy as jnp
from jax import lax
from jax.experimental import pallas as pl
from jax.experimental.pallas import tpu as pltpu
from jax.sharding import PartitionSpec as P


HD = 128
BLOCK = 128
LEN_BLOCKS = 11
EPSILON = 1e-06
THETA = 1000000.0
HBM = pltpu.MemorySpace.HBM
VMEM = pltpu.MemorySpace.VMEM
SMEM = pltpu.MemorySpace.SMEM
MIB = 1024 * 1024


def ring(block, axis, hop, last_ahead, tied=None):
    size = lax.axis_size(axis)
    count = size // hop
    ahead = [(i, (i + hop) % size) for i in range(size)]
    back = [(i, (i - hop) % size) for i in range(size)]
    got = {0: block}
    up = down = block
    for step in range(1, count // 2):
        up = lax.ppermute(up, axis, ahead)
        down = lax.ppermute(down, axis, back)
        got[count - step] = up
        got[step] = down
        if tied and step == 1:
            up, *tied[:] = lax.optimization_barrier((up, *tied))
    if last_ahead:
        got[count // 2] = lax.ppermute(up, axis, ahead)
    else:
        got[count // 2] = lax.ppermute(down, axis, back)
    return [got[i] for i in range(count)]


def swap(block, axis):
    size = lax.axis_size(axis)
    return lax.ppermute(block, axis, [(i, i ^ 1) for i in range(size)])


def by_arrival(count):
    order = [0]
    for step in range(1, count // 2):
        order += [step, count - step]
    return order


def weight_copies(place, weights, wbuf, sem, count, feat, lo, width):
    tp, chip, core = place[0], place[1], place[2]
    mine, other, mine_mid, other_mid = weights
    w_rows = feat // 2
    copies = []
    for k, rel in enumerate([*by_arrival(count), count // 2]):
        i = jnp.bitwise_and(chip + rel - tp, count - 1)
        for which in range(2):
            spot = core if which == 0 else 1 - core
            if rel == count // 2:
                src = mine_mid if which == 0 else other_mid
            else:
                src = (mine if which == 0 else other).at[k]
            copies.append(
                pltpu.make_async_copy(
                    src.at[pl.ds(0, w_rows), pl.ds(lo, width)],
                    wbuf.at[pl.ds(pl.multiple_of(i * feat + spot * w_rows, 64), w_rows)],
                    sem.at[2 * rel + which],
                )
            )
    return copies


def rotated(head, cos, sin):
    return (head * cos[...] + pltpu.roll(head, HD // 2, 1) * sin[...]).astype(jnp.bfloat16)


def normalize(pieces, gain, out):
    rows, feat = pieces[0].shape
    tile = 32

    def one_tile(r, unused):
        at_rows = pl.ds(pl.multiple_of(r * tile, tile), tile)
        totals = [jnp.zeros((tile, 128), jnp.float32) for _ in range(2)]
        for piece in pieces:
            for g in range(feat // 128):
                part = piece[at_rows, g * 128 : (g + 1) * 128].astype(jnp.float32)
                totals[g % 2] = totals[g % 2] + part * part
        mean = jnp.sum(totals[0] + totals[1], axis=1, keepdims=True) * (1.0 / (feat * len(pieces)))
        scale = jnp.broadcast_to(lax.rsqrt(mean + EPSILON), (tile, 128))
        for i, piece in enumerate(pieces):
            for g in range(feat // 128):
                part = piece[at_rows, g * 128 : (g + 1) * 128].astype(jnp.float32)
                at_col = slice(i * feat + g * 128, i * feat + (g + 1) * 128)
                out[at_rows, at_col] = (part * scale * gain[:, at_col]).astype(jnp.bfloat16)
        return unused

    lax.fori_loop(0, rows // tile, one_tile, 0)


def norm_kernel(*refs):
    normalize(refs[:-2], refs[-2], refs[-1])


def norm_rows(pieces, gain):
    count = len(pieces)
    rows, feat = pieces[0].shape
    return pl.pallas_call(
        norm_kernel,
        out_shape=jax.ShapeDtypeStruct((rows, count * feat), jnp.bfloat16),
        in_specs=[pl.BlockSpec(memory_space=VMEM)] * (count + 1),
        out_specs=pl.BlockSpec(memory_space=VMEM),
        compiler_params=pltpu.CompilerParams(vmem_limit_bytes=12 * MIB),
        cost_estimate=pl.CostEstimate(
            flops=6 * rows * feat * count, bytes_accessed=4 * rows * feat * count, transcendentals=0
        ),
    )(*pieces, gain)


def keys_kernel(place, x_a, *refs, count, feat, lo):
    pieces = refs[:count]
    weights = refs[count : count + 4]
    gain, cos, sin, kv, labels, x_b = refs[count + 4 : count + 10]
    wbuf, acc, tags, sem_w, sem_tag = refs[count + 10 :]
    w_rows = feat // 2
    mid = count // 2
    part = x_a.shape[0]
    w_copies = weight_copies(place, weights, wbuf, sem_w, count, feat, lo, 2 * HD)
    t_copies = []
    for which in range(2):
        for k, rel in enumerate([*by_arrival(count), mid]):
            src = weights[2 + which] if rel == mid else weights[which].at[k]
            t_copies.append(
                pltpu.make_async_copy(
                    src.at[pl.ds(w_rows, 8), pl.ds(0, 128)],
                    tags.at[which * count + rel],
                    sem_tag.at[which * count + rel],
                )
            )
    for copy in w_copies + t_copies:
        copy.start()
    normalize(pieces, gain, x_b)
    for copy in w_copies + t_copies:
        copy.wait()
    acc[:part] = jnp.dot(x_a[...], wbuf[...], preferred_element_type=jnp.float32)
    acc[part:] = jnp.dot(x_b[...], wbuf[...], preferred_element_type=jnp.float32)
    kv[:, :HD] = rotated(acc[:, :HD], cos, sin)
    kv[:, HD:] = acc[:, HD:].astype(jnp.bfloat16)
    for r in range(2 * count):
        labels[r : r + 1, :] = tags[r].astype(jnp.float32)[0:1].astype(jnp.int32)


def queries_kernel(place, x_a, x_b, mine, other, mine_mid, other_mid, cos, sin, q, wbuf, acc, sem_w, *, count, feat, heads):
    part = x_a.shape[0]
    weights = (mine, other, mine_mid, other_mid)
    w_copies = weight_copies(place, weights, wbuf, sem_w, count, feat, 0, heads * HD)
    for copy in w_copies:
        copy.start()
    for copy in w_copies:
        copy.wait()
    for half, x in enumerate((x_a, x_b)):
        rows = pl.ds(half * part, part)
        acc[...] = jnp.dot(x[...], wbuf[...], preferred_element_type=jnp.float32)
        for h in range(heads):
            q[h, rows] = rotated(acc[:, h * HD : (h + 1) * HD], cos.at[rows], sin.at[rows])


def project_keys(place, x_a, pieces, weights, gain, cos, sin, lo):
    count = len(pieces)
    part, feat = pieces[0].shape
    tok = 2 * part
    return pl.pallas_call(
        functools.partial(keys_kernel, count=count, feat=feat, lo=lo),
        out_shape=(
            jax.ShapeDtypeStruct((tok, 2 * HD), jnp.bfloat16),
            jax.ShapeDtypeStruct((2 * count, 128), jnp.int32),
            jax.ShapeDtypeStruct((part, count * feat), jnp.bfloat16),
        ),
        in_specs=[pl.BlockSpec(memory_space=SMEM)]
        + [pl.BlockSpec(memory_space=VMEM)] * (count + 1)
        + [pl.BlockSpec(memory_space=HBM)]
        + [pl.BlockSpec(memory_space=pl.ANY)] * 3
        + [pl.BlockSpec(memory_space=VMEM)] * 3,
        out_specs=(pl.BlockSpec(memory_space=VMEM),) * 3,
        scratch_shapes=[
            pltpu.VMEM((count * feat, 2 * HD), jnp.bfloat16),
            pltpu.VMEM((tok, 2 * HD), jnp.float32),
            pltpu.VMEM((2 * count, 8, 128), jnp.bfloat16),
            pltpu.SemaphoreType.DMA((2 * count,)),
            pltpu.SemaphoreType.DMA((2 * count,)),
        ],
        compiler_params=pltpu.CompilerParams(vmem_limit_bytes=20 * MIB),
        cost_estimate=pl.CostEstimate(
            flops=4 * tok * feat * count * HD, bytes_accessed=4 * tok * feat * count, transcendentals=0
        ),
    )(place, x_a, *pieces, *weights, gain, cos, sin)


def project_queries(place, x_a, x_b, weights, cos, sin, heads):
    count = weights[0].shape[0] + 1
    part = x_a.shape[0]
    tok = 2 * part
    feat = x_a.shape[1] // count
    width = heads * HD
    return pl.pallas_call(
        functools.partial(queries_kernel, count=count, feat=feat, heads=heads),
        out_shape=jax.ShapeDtypeStruct((heads, tok, HD), jnp.bfloat16),
        in_specs=[pl.BlockSpec(memory_space=SMEM)]
        + [pl.BlockSpec(memory_space=VMEM)] * 2
        + [pl.BlockSpec(memory_space=HBM)]
        + [pl.BlockSpec(memory_space=pl.ANY)] * 3
        + [pl.BlockSpec(memory_space=VMEM)] * 2,
        out_specs=pl.BlockSpec(memory_space=VMEM),
        scratch_shapes=[
            pltpu.VMEM((count * feat, width), jnp.bfloat16),
            pltpu.VMEM((part, width), jnp.float32),
            pltpu.SemaphoreType.DMA((2 * count,)),
        ],
        compiler_params=pltpu.CompilerParams(vmem_limit_bytes=20 * MIB),
        cost_estimate=pl.CostEstimate(
            flops=2 * tok * feat * count * width, bytes_accessed=2 * tok * feat * count, transcendentals=0
        ),
    )(place, x_a, x_b, *weights, cos, sin)


def attend_kernel(
    info, q_in, far, near, own, *refs, lo, hi
):
    out, qbuf, kvbuf, sbuf, mbuf, lbuf, obuf, tbuf, sems, sem_out = refs[-10:]
    heads = q_in.shape[0]
    tok = own.shape[0]
    local = tok // BLOCK
    back = 2 * local
    span_in = pl.ds(lo * BLOCK, (hi - lo) * BLOCK)
    copies = [
        pltpu.make_async_copy(q_in.at[:, span_in], qbuf.at[:, span_in], sems.at[0]),
        pltpu.make_async_copy(far, kvbuf.at[pl.ds(BLOCK, tok)], sems.at[1]),
        pltpu.make_async_copy(near, kvbuf.at[pl.ds(BLOCK + tok, tok)], sems.at[2]),
        pltpu.make_async_copy(own, kvbuf.at[pl.ds(BLOCK + 2 * tok, tok)], sems.at[3]),
    ]
    for copy in copies:
        copy.start()
    kvbuf[:BLOCK] = jnp.zeros((BLOCK, 2 * HD), jnp.bfloat16)
    for copy in copies:
        copy.wait()
    first = info[0]
    n_prompts = info.shape[0] - 1
    factor = math.log2(math.e) / math.sqrt(HD)
    rows = heads * BLOCK
    row = lax.broadcasted_iota(jnp.int32, (BLOCK, BLOCK), 0)
    col = lax.broadcasted_iota(jnp.int32, (BLOCK, BLOCK), 1)
    causal = col <= row

    def result_copy(i):
        at = pl.ds(pl.multiple_of(i * BLOCK, BLOCK), BLOCK)
        return pltpu.make_async_copy(tbuf.at[i - lo], out.at[at], sem_out.at[i - lo])

    def one_block(i, unused):
        block = first + i

        def find(p, state):
            start, best = state
            best = jnp.where(start <= block, start, best)
            return start + info[1 + p], best

        _, begin = lax.fori_loop(0, n_prompts, find, (jnp.int32(0), jnp.int32(0)))
        low = jnp.maximum(begin - first + back, i) + 1
        last = back + i + 1
        pairs = (last - low + 2) // 2
        q = qbuf[:, pl.ds(pl.multiple_of(i * BLOCK, BLOCK), BLOCK), :].reshape(rows, HD)

        def span(t):
            return pl.ds(pl.multiple_of((last - 1 - 2 * t) * BLOCK, BLOCK), 2 * BLOCK)

        def score(t, h):
            s = lax.dot_general(
                q[h * BLOCK : (h + 1) * BLOCK],
                kvbuf[span(t), :HD],
                (((1,), (1,)), ((), ())),
                preferred_element_type=jnp.float32,
            )
            inside = last - 1 - 2 * t >= low
            bias = jnp.where(inside, 0.0, -1e30)
            return s[:, :BLOCK] * factor + bias, s[:, BLOCK:] * factor

        mbuf[...] = jnp.full_like(mbuf, -1e30)

        def upward(t, unused):
            shut = jnp.where(t == 0, -1e30, 0.0)
            for h in range(heads):
                at = slice(h * BLOCK, (h + 1) * BLOCK)
                left, right = score(t, h)
                right = right + jnp.where(causal, 0.0, shut)
                sbuf[t, at, :BLOCK] = left
                sbuf[t, at, BLOCK:] = right
                mbuf[at] = jnp.maximum(mbuf[at], jnp.maximum(left, right))
            return unused

        lax.fori_loop(0, pairs, upward, 0)
        top = jnp.max(mbuf[...], axis=1, keepdims=True)
        mbuf[...] = jnp.broadcast_to(top, mbuf.shape)
        lbuf[...] = jnp.zeros_like(lbuf)
        obuf[...] = jnp.zeros_like(obuf)

        def gather(t, unused):
            for h in range(heads):
                at = slice(h * BLOCK, (h + 1) * BLOCK)
                peak = mbuf[at]
                left = jnp.exp2(sbuf[t, at, :BLOCK] - peak)
                right = jnp.exp2(sbuf[t, at, BLOCK:] - peak)
                lbuf[at] += left + right
                p = jnp.concatenate([left.astype(jnp.bfloat16), right.astype(jnp.bfloat16)], axis=1)
                obuf[at] += jnp.dot(p, kvbuf[span(t), HD:], preferred_element_type=jnp.float32)
            return unused

        lax.fori_loop(0, pairs, gather, 0)
        total = jnp.sum(lbuf[...], axis=1, keepdims=True)
        result = (obuf[...] / total).astype(jnp.bfloat16)
        for h in range(heads):
            tbuf[i - lo, :, h * HD : (h + 1) * HD] = result[h * BLOCK : (h + 1) * BLOCK]
        result_copy(i).start()
        return unused

    lax.fori_loop(lo, hi, one_block, 0)
    for i in range(lo, hi):
        result_copy(i).wait()


def attend(info, q, far, near, own, lo, hi, base=None):
    heads = q.shape[0]
    tok = own.shape[0]
    operands = [info, q, far, near, own]
    if base is not None:
        operands.append(base)
    return pl.pallas_call(
        functools.partial(attend_kernel, lo=lo, hi=hi),
        out_shape=jax.ShapeDtypeStruct((tok, heads * HD), jnp.bfloat16),
        in_specs=[pl.BlockSpec(memory_space=SMEM)]
        + [pl.BlockSpec(memory_space=pl.ANY)] * (len(operands) - 1),
        out_specs=pl.BlockSpec(memory_space=pl.ANY),
        scratch_shapes=[
            pltpu.VMEM((heads, tok, HD), jnp.bfloat16),
            pltpu.VMEM((3 * tok + BLOCK, 2 * HD), jnp.bfloat16),
            pltpu.VMEM(((LEN_BLOCKS + 1) // 2, heads * BLOCK, 2 * BLOCK), jnp.float32),
            pltpu.VMEM((heads * BLOCK, BLOCK), jnp.float32),
            pltpu.VMEM((heads * BLOCK, BLOCK), jnp.float32),
            pltpu.VMEM((heads * BLOCK, HD), jnp.float32),
            pltpu.VMEM((hi - lo, BLOCK, heads * HD), jnp.bfloat16),
            pltpu.SemaphoreType.DMA((4,)),
            pltpu.SemaphoreType.DMA((hi - lo,)),
        ],
        input_output_aliases={5: 0} if base is not None else {},
        compiler_params=pltpu.CompilerParams(vmem_limit_bytes=12 * MIB),
        cost_estimate=pl.CostEstimate(
            flops=2 * 10**9 * (hi - lo), bytes_accessed=4 * 10**6, transcendentals=10**6
        ),
    )(*operands)


def cache_kernel(place, labels, table, mine, other, mine_mid, other_mid, out, sem, *, local, count, tok):
    chip, core, me = place[1], place[2], place[3]
    mid = count // 2
    slots = out.shape[0]

    def put(src, at_row, slot):
        return pltpu.make_async_copy(src.at[pl.ds(pl.multiple_of(at_row, BLOCK), BLOCK)], out.at[slot], sem)

    def one(source, rank):
        rel = jnp.bitwise_and(jnp.right_shift(source, 1) - chip, count - 1)
        same = jnp.bitwise_and(source, 1) == core
        middle = rel == mid
        spot = jnp.where(rel > mid, 2 * (count - rel), jnp.where(middle, 0, jnp.maximum(2 * rel - 1, 0)))
        label_row = jnp.where(same, rel, count + rel)
        for inner in range(local):
            hit = labels[label_row, inner] == me

            @pl.when(hit)
            def _():
                slot = table[0, rank]
                at_row = spot * tok + inner * BLOCK

                @pl.when(same & jnp.logical_not(middle))
                def _():
                    put(mine, at_row, slot).start()

                @pl.when(jnp.logical_not(same) & jnp.logical_not(middle))
                def _():
                    put(other, at_row, slot).start()

                @pl.when(same & middle)
                def _():
                    put(mine_mid, at_row, slot).start()

                @pl.when(jnp.logical_not(same) & middle)
                def _():
                    put(other_mid, at_row, slot).start()

            rank = rank + hit.astype(jnp.int32)
        return rank

    found = lax.fori_loop(0, 2 * count, one, jnp.int32(0))

    def clear(r, unused):
        out[table[0, r]] = jnp.zeros(out.shape[1:], out.dtype)
        return unused

    lax.fori_loop(found, slots, clear, 0)

    def settle(r, unused):
        put(mine, 0, 0).wait()
        return unused

    lax.fori_loop(0, found, settle, 0)


def fill_cache(place, labels, table, mine, other, mine_mid, other_mid, local, count):
    tok = mine_mid.shape[0]
    slots = table.shape[1]
    return pl.pallas_call(
        functools.partial(cache_kernel, local=local, count=count, tok=tok),
        out_shape=jax.ShapeDtypeStruct((slots, BLOCK, mine.shape[1]), jnp.bfloat16),
        in_specs=[pl.BlockSpec(memory_space=SMEM)] * 3 + [pl.BlockSpec(memory_space=pl.ANY)] * 4,
        out_specs=pl.BlockSpec(memory_space=VMEM),
        scratch_shapes=[pltpu.SemaphoreType.DMA],
        compiler_params=pltpu.CompilerParams(vmem_limit_bytes=8 * MIB),
    )(place, labels, table, mine, other, mine_mid, other_mid)


def on_device(
    hidden_states, norm_gain, w_query, w_key, w_value, prompt_blocks, owner_map, slot_table
):
    tok, feat = hidden_states.shape
    n_dev = lax.axis_size("dev")
    n_tp = lax.axis_size("tp")
    device = lax.axis_index("dev")
    count = n_dev // 2
    assert count & (count - 1) == 0 and count == n_tp
    mid = count // 2
    local = tok // BLOCK
    heads = w_query.shape[1] // HD
    place = jnp.stack([lax.axis_index("tp"), device // 2, device % 2, device]).astype(jnp.int32)

    token_rows = device * tok + jnp.arange(tok, dtype=jnp.int32)
    starts = (jnp.cumsum(prompt_blocks) - prompt_blocks) * BLOCK
    start_of = jnp.max(jnp.where(token_rows[:, None] >= starts[None, :], starts[None, :], 0), axis=1)
    offsets = token_rows - start_of
    lane = jnp.arange(HD, dtype=jnp.int32)
    freq_index = lax.rem(lane, HD // 2).astype(jnp.float32)
    inverse = jnp.exp(freq_index * (-2.0 * math.log(THETA) / HD))
    angles = offsets.astype(jnp.float32)[:, None] * inverse[None, :]
    cos = jnp.cos(angles)
    sin = jnp.sin(angles) * jnp.where(lane < HD // 2, -1.0, 1.0)[None, :]
    gain = norm_gain.astype(jnp.float32)
    gain = lax.dynamic_slice_in_dim(
        jnp.concatenate([gain, gain]), lax.axis_index("tp") * feat, n_tp * feat
    )[None]
    info = jnp.concatenate([(device * local)[None].astype(jnp.int32), prompt_blocks])

    part = tok // 2
    tied = [cos, sin, gain, place, info]
    x_a = ring(hidden_states[:part], "tp", 1, True)
    x_b = ring(hidden_states[part:], "tp", 1, False, tied)
    cos, sin, gain, place, info = tied

    weights = jnp.concatenate([w_query, w_key, w_value], axis=1)
    w_cols = weights.shape[1]
    labels = jnp.pad(owner_map.astype(jnp.bfloat16)[None], ((0, 7), (0, w_cols - local)))
    weights = jnp.concatenate([weights, labels], axis=0)
    arrival = by_arrival(count)
    w_got = ring(weights, "dev", 2, True)
    w_mine = jnp.stack([w_got[i] for i in arrival])
    w_other = swap(w_mine, "dev")
    w_other_mid = swap(w_got[mid], "dev")
    w_set = (w_mine, w_other, w_got[mid], w_other_mid)

    n_a = norm_rows(x_a, gain)
    kv, labels, n_b = project_keys(place, n_a, x_b, w_set, gain, cos, sin, heads * HD)
    q = project_queries(place, n_a, n_b, w_set, cos, sin, heads)

    near = lax.ppermute(kv, "dev", [(i, i + 1) for i in range(n_dev - 1)])
    k_got = ring(kv, "dev", 2, False)
    far = k_got[count - 1]
    cuts = (0, local // 2, local - 1, local)
    context = attend(info, q, far, near, kv, cuts[0], cuts[1])
    context = attend(info, q, far, near, kv, cuts[1], cuts[2], base=context)
    context = attend(info, q, far, near, kv, cuts[2], cuts[3], base=context)
    k_mine = jnp.concatenate([k_got[i] for i in arrival], axis=0)
    k_other = swap(k_mine, "dev")
    k_mid_other = swap(k_got[mid], "dev")
    kv_cache = fill_cache(
        place, labels, slot_table, k_mine, k_other, k_got[mid], k_mid_other, local, count
    )
    return (context, kv_cache)


def solution(mesh):
    in_specs = (
        P(("groups", "dev"), "tp"),
        P(),
        P("dev", "tp"),
        P("dev", "tp"),
        P("dev", "tp"),
        P("groups"),
        P(("groups", "dev")),
        P(("groups", "dev"), None),
    )
    out_specs = (P(("groups", "dev"), "tp"), P(("groups", "dev"), None, "tp"))

    return jax.shard_map(on_device, mesh=mesh, in_specs=in_specs, out_specs=out_specs, check_vma=False)
```

```python
import functools
import math

import jax
import jax.numpy as jnp
from jax import lax
from jax.experimental import pallas as pl
from jax.experimental.pallas import tpu as pltpu
from jax.sharding import PartitionSpec as P


HD = 128
BLOCK = 128
LEN_BLOCKS = 11
EPSILON = 1e-06
THETA = 1000000.0
HBM = pltpu.MemorySpace.HBM
VMEM = pltpu.MemorySpace.VMEM
SMEM = pltpu.MemorySpace.SMEM
MIB = 1024 * 1024


def ring(block, axis, hop, last_ahead, tied=None):
    size = lax.axis_size(axis)
    count = size // hop
    ahead = [(i, (i + hop) % size) for i in range(size)]
    back = [(i, (i - hop) % size) for i in range(size)]
    got = {0: block}
    up = down = block
    for step in range(1, count // 2):
        up = lax.ppermute(up, axis, ahead)
        down = lax.ppermute(down, axis, back)
        got[count - step] = up
        got[step] = down
        if tied and step == 1:
            up, *tied[:] = lax.optimization_barrier((up, *tied))
    if last_ahead:
        got[count // 2] = lax.ppermute(up, axis, ahead)
    else:
        got[count // 2] = lax.ppermute(down, axis, back)
    return [got[i] for i in range(count)]


def swap(block, axis):
    size = lax.axis_size(axis)
    return lax.ppermute(block, axis, [(i, i ^ 1) for i in range(size)])


def by_arrival(count):
    order = [0]
    for step in range(1, count // 2):
        order += [step, count - step]
    return order


def weight_copies(place, weights, wbuf, sem, count, feat, lo, width):
    tp, chip, core = place[0], place[1], place[2]
    mine, other, mine_mid, other_mid = weights
    w_rows = feat // 2
    copies = []
    for k, rel in enumerate([*by_arrival(count), count // 2]):
        i = jnp.bitwise_and(chip + rel - tp, count - 1)
        for which in range(2):
            spot = core if which == 0 else 1 - core
            if rel == count // 2:
                src = mine_mid if which == 0 else other_mid
            else:
                src = (mine if which == 0 else other).at[k]
            copies.append(
                pltpu.make_async_copy(
                    src.at[pl.ds(0, w_rows), pl.ds(lo, width)],
                    wbuf.at[pl.ds(pl.multiple_of(i * feat + spot * w_rows, 64), w_rows)],
                    sem.at[2 * rel + which],
                )
            )
    return copies


def rotated(head, cos, sin):
    return (head * cos[...] + pltpu.roll(head, HD // 2, 1) * sin[...]).astype(jnp.bfloat16)


def normalize(pieces, gain, out):
    rows, feat = pieces[0].shape
    tile = 32

    def one_tile(r, unused):
        at_rows = pl.ds(pl.multiple_of(r * tile, tile), tile)
        totals = [jnp.zeros((tile, 128), jnp.float32) for _ in range(2)]
        for piece in pieces:
            for g in range(feat // 128):
                part = piece[at_rows, g * 128 : (g + 1) * 128].astype(jnp.float32)
                totals[g % 2] = totals[g % 2] + part * part
        mean = jnp.sum(totals[0] + totals[1], axis=1, keepdims=True) * (1.0 / (feat * len(pieces)))
        scale = jnp.broadcast_to(lax.rsqrt(mean + EPSILON), (tile, 128))
        for i, piece in enumerate(pieces):
            for g in range(feat // 128):
                part = piece[at_rows, g * 128 : (g + 1) * 128].astype(jnp.float32)
                at_col = slice(i * feat + g * 128, i * feat + (g + 1) * 128)
                out[at_rows, at_col] = (part * scale * gain[:, at_col]).astype(jnp.bfloat16)
        return unused

    lax.fori_loop(0, rows // tile, one_tile, 0)


def norm_kernel(*refs):
    normalize(refs[:-2], refs[-2], refs[-1])


def norm_rows(pieces, gain):
    count = len(pieces)
    rows, feat = pieces[0].shape
    return pl.pallas_call(
        norm_kernel,
        out_shape=jax.ShapeDtypeStruct((rows, count * feat), jnp.bfloat16),
        in_specs=[pl.BlockSpec(memory_space=VMEM)] * (count + 1),
        out_specs=pl.BlockSpec(memory_space=VMEM),
        compiler_params=pltpu.CompilerParams(vmem_limit_bytes=12 * MIB),
        cost_estimate=pl.CostEstimate(
            flops=6 * rows * feat * count, bytes_accessed=4 * rows * feat * count, transcendentals=0
        ),
    )(*pieces, gain)


def keys_kernel(place, x_a, *refs, count, feat, lo):
    pieces = refs[:count]
    weights = refs[count : count + 4]
    gain, cos, sin, kv, labels, x_b = refs[count + 4 : count + 10]
    wbuf, acc, tags, sem_w, sem_tag = refs[count + 10 :]
    w_rows = feat // 2
    mid = count // 2
    part = x_a.shape[0]
    w_copies = weight_copies(place, weights, wbuf, sem_w, count, feat, lo, 2 * HD)
    t_copies = []
    for which in range(2):
        for k, rel in enumerate([*by_arrival(count), mid]):
            src = weights[2 + which] if rel == mid else weights[which].at[k]
            t_copies.append(
                pltpu.make_async_copy(
                    src.at[pl.ds(w_rows, 8), pl.ds(0, 128)],
                    tags.at[which * count + rel],
                    sem_tag.at[which * count + rel],
                )
            )
    for copy in w_copies + t_copies:
        copy.start()
    normalize(pieces, gain, x_b)
    for copy in w_copies + t_copies:
        copy.wait()
    acc[:part] = jnp.dot(x_a[...], wbuf[...], preferred_element_type=jnp.float32)
    acc[part:] = jnp.dot(x_b[...], wbuf[...], preferred_element_type=jnp.float32)
    kv[:, :HD] = rotated(acc[:, :HD], cos, sin)
    kv[:, HD:] = acc[:, HD:].astype(jnp.bfloat16)
    for r in range(2 * count):
        labels[r : r + 1, :] = tags[r].astype(jnp.float32)[0:1].astype(jnp.int32)


def queries_kernel(place, x_a, x_b, mine, other, mine_mid, other_mid, cos, sin, q, wbuf, acc, sem_w, *, count, feat, heads):
    part = x_a.shape[0]
    weights = (mine, other, mine_mid, other_mid)
    w_copies = weight_copies(place, weights, wbuf, sem_w, count, feat, 0, heads * HD)
    for copy in w_copies:
        copy.start()
    for copy in w_copies:
        copy.wait()
    for half, x in enumerate((x_a, x_b)):
        rows = pl.ds(half * part, part)
        acc[...] = jnp.dot(x[...], wbuf[...], preferred_element_type=jnp.float32)
        for h in range(heads):
            q[h, rows] = rotated(acc[:, h * HD : (h + 1) * HD], cos.at[rows], sin.at[rows])


def project_keys(place, x_a, pieces, weights, gain, cos, sin, lo):
    count = len(pieces)
    part, feat = pieces[0].shape
    tok = 2 * part
    return pl.pallas_call(
        functools.partial(keys_kernel, count=count, feat=feat, lo=lo),
        out_shape=(
            jax.ShapeDtypeStruct((tok, 2 * HD), jnp.bfloat16),
            jax.ShapeDtypeStruct((2 * count, 128), jnp.int32),
            jax.ShapeDtypeStruct((part, count * feat), jnp.bfloat16),
        ),
        in_specs=[pl.BlockSpec(memory_space=SMEM)]
        + [pl.BlockSpec(memory_space=VMEM)] * (count + 1)
        + [pl.BlockSpec(memory_space=HBM)]
        + [pl.BlockSpec(memory_space=pl.ANY)] * 3
        + [pl.BlockSpec(memory_space=VMEM)] * 3,
        out_specs=(pl.BlockSpec(memory_space=VMEM),) * 3,
        scratch_shapes=[
            pltpu.VMEM((count * feat, 2 * HD), jnp.bfloat16),
            pltpu.VMEM((tok, 2 * HD), jnp.float32),
            pltpu.VMEM((2 * count, 8, 128), jnp.bfloat16),
            pltpu.SemaphoreType.DMA((2 * count,)),
            pltpu.SemaphoreType.DMA((2 * count,)),
        ],
        compiler_params=pltpu.CompilerParams(vmem_limit_bytes=20 * MIB),
        cost_estimate=pl.CostEstimate(
            flops=4 * tok * feat * count * HD, bytes_accessed=4 * tok * feat * count, transcendentals=0
        ),
    )(place, x_a, *pieces, *weights, gain, cos, sin)


def project_queries(place, x_a, x_b, weights, cos, sin, heads):
    count = weights[0].shape[0] + 1
    part = x_a.shape[0]
    tok = 2 * part
    feat = x_a.shape[1] // count
    width = heads * HD
    return pl.pallas_call(
        functools.partial(queries_kernel, count=count, feat=feat, heads=heads),
        out_shape=jax.ShapeDtypeStruct((heads, tok, HD), jnp.bfloat16),
        in_specs=[pl.BlockSpec(memory_space=SMEM)]
        + [pl.BlockSpec(memory_space=VMEM)] * 2
        + [pl.BlockSpec(memory_space=HBM)]
        + [pl.BlockSpec(memory_space=pl.ANY)] * 3
        + [pl.BlockSpec(memory_space=VMEM)] * 2,
        out_specs=pl.BlockSpec(memory_space=VMEM),
        scratch_shapes=[
            pltpu.VMEM((count * feat, width), jnp.bfloat16),
            pltpu.VMEM((part, width), jnp.float32),
            pltpu.SemaphoreType.DMA((2 * count,)),
        ],
        compiler_params=pltpu.CompilerParams(vmem_limit_bytes=20 * MIB),
        cost_estimate=pl.CostEstimate(
            flops=2 * tok * feat * count * width, bytes_accessed=2 * tok * feat * count, transcendentals=0
        ),
    )(place, x_a, x_b, *weights, cos, sin)


def attend_kernel(
    info, q_in, far, near, own, *refs, lo, hi
):
    out, qbuf, kvbuf, sbuf, mbuf, lbuf, obuf, tbuf, sems, sem_out = refs[-10:]
    heads = q_in.shape[0]
    tok = own.shape[0]
    local = tok // BLOCK
    back = 2 * local
    span_in = pl.ds(lo * BLOCK, (hi - lo) * BLOCK)
    copies = [
        pltpu.make_async_copy(q_in.at[:, span_in], qbuf.at[:, span_in], sems.at[0]),
        pltpu.make_async_copy(far, kvbuf.at[pl.ds(BLOCK, tok)], sems.at[1]),
        pltpu.make_async_copy(near, kvbuf.at[pl.ds(BLOCK + tok, tok)], sems.at[2]),
        pltpu.make_async_copy(own, kvbuf.at[pl.ds(BLOCK + 2 * tok, tok)], sems.at[3]),
    ]
    for copy in copies:
        copy.start()
    kvbuf[:BLOCK] = jnp.zeros((BLOCK, 2 * HD), jnp.bfloat16)
    for copy in copies:
        copy.wait()
    first = info[0]
    n_prompts = info.shape[0] - 1
    factor = math.log2(math.e) / math.sqrt(HD)
    rows = heads * BLOCK
    row = lax.broadcasted_iota(jnp.int32, (BLOCK, BLOCK), 0)
    col = lax.broadcasted_iota(jnp.int32, (BLOCK, BLOCK), 1)
    causal = col <= row

    def result_copy(i):
        at = pl.ds(pl.multiple_of(i * BLOCK, BLOCK), BLOCK)
        return pltpu.make_async_copy(tbuf.at[i - lo], out.at[at], sem_out.at[i - lo])

    def one_block(i, unused):
        block = first + i

        def find(p, state):
            start, best = state
            best = jnp.where(start <= block, start, best)
            return start + info[1 + p], best

        _, begin = lax.fori_loop(0, n_prompts, find, (jnp.int32(0), jnp.int32(0)))
        low = jnp.maximum(begin - first + back, i) + 1
        last = back + i + 1
        pairs = (last - low + 2) // 2
        q = qbuf[:, pl.ds(pl.multiple_of(i * BLOCK, BLOCK), BLOCK), :].reshape(rows, HD)

        def span(t):
            return pl.ds(pl.multiple_of((last - 1 - 2 * t) * BLOCK, BLOCK), 2 * BLOCK)

        def score(t, h):
            s = lax.dot_general(
                q[h * BLOCK : (h + 1) * BLOCK],
                kvbuf[span(t), :HD],
                (((1,), (1,)), ((), ())),
                preferred_element_type=jnp.float32,
            )
            inside = last - 1 - 2 * t >= low
            bias = jnp.where(inside, 0.0, -1e30)
            return s[:, :BLOCK] * factor + bias, s[:, BLOCK:] * factor

        mbuf[...] = jnp.full_like(mbuf, -1e30)

        def upward(t, unused):
            shut = jnp.where(t == 0, -1e30, 0.0)
            for h in range(heads):
                at = slice(h * BLOCK, (h + 1) * BLOCK)
                left, right = score(t, h)
                right = right + jnp.where(causal, 0.0, shut)
                sbuf[t, at, :BLOCK] = left
                sbuf[t, at, BLOCK:] = right
                mbuf[at] = jnp.maximum(mbuf[at], jnp.maximum(left, right))
            return unused

        lax.fori_loop(0, pairs, upward, 0)
        top = jnp.max(mbuf[...], axis=1, keepdims=True)
        mbuf[...] = jnp.broadcast_to(top, mbuf.shape)
        lbuf[...] = jnp.zeros_like(lbuf)
        obuf[...] = jnp.zeros_like(obuf)

        def gather(t, unused):
            for h in range(heads):
                at = slice(h * BLOCK, (h + 1) * BLOCK)
                peak = mbuf[at]
                left = jnp.exp2(sbuf[t, at, :BLOCK] - peak)
                right = jnp.exp2(sbuf[t, at, BLOCK:] - peak)
                lbuf[at] += left + right
                p = jnp.concatenate([left.astype(jnp.bfloat16), right.astype(jnp.bfloat16)], axis=1)
                obuf[at] += jnp.dot(p, kvbuf[span(t), HD:], preferred_element_type=jnp.float32)
            return unused

        lax.fori_loop(0, pairs, gather, 0)
        total = jnp.sum(lbuf[...], axis=1, keepdims=True)
        result = (obuf[...] / total).astype(jnp.bfloat16)
        for h in range(heads):
            tbuf[i - lo, :, h * HD : (h + 1) * HD] = result[h * BLOCK : (h + 1) * BLOCK]
        result_copy(i).start()
        return unused

    lax.fori_loop(lo, hi, one_block, 0)
    for i in range(lo, hi):
        result_copy(i).wait()


def attend(info, q, far, near, own, lo, hi, base=None):
    heads = q.shape[0]
    tok = own.shape[0]
    operands = [info, q, far, near, own]
    if base is not None:
        operands.append(base)
    return pl.pallas_call(
        functools.partial(attend_kernel, lo=lo, hi=hi),
        out_shape=jax.ShapeDtypeStruct((tok, heads * HD), jnp.bfloat16),
        in_specs=[pl.BlockSpec(memory_space=SMEM)]
        + [pl.BlockSpec(memory_space=pl.ANY)] * (len(operands) - 1),
        out_specs=pl.BlockSpec(memory_space=pl.ANY),
        scratch_shapes=[
            pltpu.VMEM((heads, tok, HD), jnp.bfloat16),
            pltpu.VMEM((3 * tok + BLOCK, 2 * HD), jnp.bfloat16),
            pltpu.VMEM(((LEN_BLOCKS + 1) // 2, heads * BLOCK, 2 * BLOCK), jnp.float32),
            pltpu.VMEM((heads * BLOCK, BLOCK), jnp.float32),
            pltpu.VMEM((heads * BLOCK, BLOCK), jnp.float32),
            pltpu.VMEM((heads * BLOCK, HD), jnp.float32),
            pltpu.VMEM((hi - lo, BLOCK, heads * HD), jnp.bfloat16),
            pltpu.SemaphoreType.DMA((4,)),
            pltpu.SemaphoreType.DMA((hi - lo,)),
        ],
        input_output_aliases={5: 0} if base is not None else {},
        compiler_params=pltpu.CompilerParams(vmem_limit_bytes=12 * MIB),
        cost_estimate=pl.CostEstimate(
            flops=2 * 10**9 * (hi - lo), bytes_accessed=4 * 10**6, transcendentals=10**6
        ),
    )(*operands)


def cache_kernel(place, labels, table, mine, other, mine_mid, other_mid, out, sem, *, local, count, tok):
    chip, core, me = place[1], place[2], place[3]
    mid = count // 2
    slots = out.shape[0]

    def put(src, at_row, slot):
        return pltpu.make_async_copy(src.at[pl.ds(pl.multiple_of(at_row, BLOCK), BLOCK)], out.at[slot], sem)

    def one(source, rank):
        rel = jnp.bitwise_and(jnp.right_shift(source, 1) - chip, count - 1)
        same = jnp.bitwise_and(source, 1) == core
        middle = rel == mid
        spot = jnp.where(rel > mid, 2 * (count - rel), jnp.where(middle, 0, jnp.maximum(2 * rel - 1, 0)))
        label_row = jnp.where(same, rel, count + rel)
        for inner in range(local):
            hit = labels[label_row, inner] == me

            @pl.when(hit)
            def _():
                slot = table[0, rank]
                at_row = spot * tok + inner * BLOCK

                @pl.when(same & jnp.logical_not(middle))
                def _():
                    put(mine, at_row, slot).start()

                @pl.when(jnp.logical_not(same) & jnp.logical_not(middle))
                def _():
                    put(other, at_row, slot).start()

                @pl.when(same & middle)
                def _():
                    put(mine_mid, at_row, slot).start()

                @pl.when(jnp.logical_not(same) & middle)
                def _():
                    put(other_mid, at_row, slot).start()

            rank = rank + hit.astype(jnp.int32)
        return rank

    found = lax.fori_loop(0, 2 * count, one, jnp.int32(0))

    def clear(r, unused):
        out[table[0, r]] = jnp.zeros(out.shape[1:], out.dtype)
        return unused

    lax.fori_loop(found, slots, clear, 0)

    def settle(r, unused):
        put(mine, 0, 0).wait()
        return unused

    lax.fori_loop(0, found, settle, 0)


def fill_cache(place, labels, table, mine, other, mine_mid, other_mid, local, count):
    tok = mine_mid.shape[0]
    slots = table.shape[1]
    return pl.pallas_call(
        functools.partial(cache_kernel, local=local, count=count, tok=tok),
        out_shape=jax.ShapeDtypeStruct((slots, BLOCK, mine.shape[1]), jnp.bfloat16),
        in_specs=[pl.BlockSpec(memory_space=SMEM)] * 3 + [pl.BlockSpec(memory_space=pl.ANY)] * 4,
        out_specs=pl.BlockSpec(memory_space=VMEM),
        scratch_shapes=[pltpu.SemaphoreType.DMA],
        compiler_params=pltpu.CompilerParams(vmem_limit_bytes=8 * MIB),
    )(place, labels, table, mine, other, mine_mid, other_mid)


def on_device(
    hidden_states, norm_gain, w_query, w_key, w_value, prompt_blocks, owner_map, slot_table
):
    tok, feat = hidden_states.shape
    n_dev = lax.axis_size("dev")
    n_tp = lax.axis_size("tp")
    device = lax.axis_index("dev")
    count = n_dev // 2
    assert count & (count - 1) == 0 and count == n_tp
    mid = count // 2
    local = tok // BLOCK
    heads = w_query.shape[1] // HD
    place = jnp.stack([lax.axis_index("tp"), device // 2, device % 2, device]).astype(jnp.int32)

    token_rows = device * tok + jnp.arange(tok, dtype=jnp.int32)
    starts = (jnp.cumsum(prompt_blocks) - prompt_blocks) * BLOCK
    start_of = jnp.max(jnp.where(token_rows[:, None] >= starts[None, :], starts[None, :], 0), axis=1)
    offsets = token_rows - start_of
    freq_index = jnp.arange(HD // 2, dtype=jnp.float32)
    inverse = jnp.exp(freq_index * (-2.0 * math.log(THETA) / HD))
    angles = offsets.astype(jnp.float32)[:, None] * inverse[None, :]
    cosine, sine = jnp.cos(angles), jnp.sin(angles)
    cos = jnp.concatenate([cosine, cosine], axis=1)
    sin = jnp.concatenate([-sine, sine], axis=1)
    gain = norm_gain.astype(jnp.float32)
    gain = lax.dynamic_slice_in_dim(
        jnp.concatenate([gain, gain]), lax.axis_index("tp") * feat, n_tp * feat
    )[None]
    info = jnp.concatenate([(device * local)[None].astype(jnp.int32), prompt_blocks])

    part = tok // 2
    tied = [cos, sin, gain, place, info]
    x_a = ring(hidden_states[:part], "tp", 1, True)
    x_b = ring(hidden_states[part:], "tp", 1, False, tied)
    cos, sin, gain, place, info = tied

    weights = jnp.concatenate([w_query, w_key, w_value], axis=1)
    w_cols = weights.shape[1]
    labels = jnp.pad(owner_map.astype(jnp.bfloat16)[None], ((0, 7), (0, w_cols - local)))
    weights = jnp.concatenate([weights, labels], axis=0)
    arrival = by_arrival(count)
    w_got = ring(weights, "dev", 2, True)
    w_mine = jnp.stack([w_got[i] for i in arrival])
    w_other = swap(w_mine, "dev")
    w_other_mid = swap(w_got[mid], "dev")
    w_set = (w_mine, w_other, w_got[mid], w_other_mid)

    n_a = norm_rows(x_a, gain)
    kv, labels, n_b = project_keys(place, n_a, x_b, w_set, gain, cos, sin, heads * HD)
    q = project_queries(place, n_a, n_b, w_set, cos, sin, heads)

    near = lax.ppermute(kv, "dev", [(i, i + 1) for i in range(n_dev - 1)])
    k_got = ring(kv, "dev", 2, False)
    far = k_got[count - 1]
    cuts = (0, local // 2, local - 1, local)
    context = attend(info, q, far, near, kv, cuts[0], cuts[1])
    context = attend(info, q, far, near, kv, cuts[1], cuts[2], base=context)
    context = attend(info, q, far, near, kv, cuts[2], cuts[3], base=context)
    k_mine = jnp.concatenate([k_got[i] for i in arrival], axis=0)
    k_other = swap(k_mine, "dev")
    k_mid_other = swap(k_got[mid], "dev")
    kv_cache = fill_cache(
        place, labels, slot_table, k_mine, k_other, k_got[mid], k_mid_other, local, count
    )
    return (context, kv_cache)


def solution(mesh):
    in_specs = (
        P(("groups", "dev"), "tp"),
        P(),
        P("dev", "tp"),
        P("dev", "tp"),
        P("dev", "tp"),
        P("groups"),
        P(("groups", "dev")),
        P(("groups", "dev"), None),
    )
    out_specs = (P(("groups", "dev"), "tp"), P(("groups", "dev"), None, "tp"))

    return jax.shard_map(on_device, mesh=mesh, in_specs=in_specs, out_specs=out_specs, check_vma=False)
```
